128 devices in a mesh: seq: 16 (over x, z), head: 8 (over y, core).
Axes of the slice: x: 4, y: 4, z: 4, core: 2. Of those that a mesh axis runs over, the one named last changes fastest.
Arguments:
- context: bfloat16 [8, 8192, 1024], P('head', 'seq'), may hold values from -6 to 6
- latents: bfloat16 [8, 1024, 1024], P('head'), may hold values from -6 to 6
- offsets: int32 [8], P('head'), may hold values from 0 to 7168
- query_gain: float32 [1024], replicated, may hold values from 0.1 to 1.9
- key_gain: float32 [1024], replicated, may hold values from 0.1 to 1.9
- layer_gain: float32 [2, 1024], replicated, may hold values from 0.1 to 1.9
- cross_query: bfloat16 [1024, 1024], P(('seq', 'head')), may hold values from -0.25 to 0.25
- cross_key: bfloat16 [1024, 1024], P(('seq', 'head')), may hold values from -0.25 to 0.25
- cross_value: bfloat16 [1024, 1024], P(('seq', 'head')), may hold values from -0.1875 to 0.1875
- cross_out: bfloat16 [1024, 1024], P(('seq', 'head')), may hold values from -0.1875 to 0.1875
- layer_qkv: bfloat16 [2, 1024, 3072], P(None, ('seq', 'head')), may hold values from -0.25 to 0.25
- layer_out: bfloat16 [2, 1024, 1024], P(None, ('seq', 'head')), may hold values from -0.1875 to 0.1875
Outputs:
- latent_out: bfloat16 [8, 1024, 1024], P('head', 'seq')
The draws below stay inside these ranges and needn't reach their ends.
Inputs may be any that keep to these rules, and one draw needn't show every extreme that they name: Latent i of row b stands at context position offsets[b] + i.
All inputs are finite; a program needn't handle non-finite values.
Results may differ from the reference program's by a relative error of at most 0.013.
Values may be sent and summed in bfloat16 or wider, within the bound.
A program may use at most 128 MiB of HBM per device.

```python
import jax
import jax.numpy as jnp
from jax import lax

D = 1024
H = 16
LATENTS = 1024
LAYERS = 2
CTX_DEV = 512
B = 8
L = 8192
N_SEQ = 16


def drawn_rows(key, salt, rows):
    return jnp.clip(jax.random.normal(jax.random.fold_in(key, salt), (B, rows, D), jnp.float32), -6.0, 6.0)


def drawn_weight(key, salt, shape):
    return jnp.clip(jax.random.normal(jax.random.fold_in(key, salt), shape, jnp.float32), -6.0, 6.0) * D ** (-0.5)


def draw_context(key, part):
    value_matrix = drawn_rows(key, 11, L)
    return value_matrix.astype(jnp.bfloat16)


def draw_latents(key, part):
    value_matrix = drawn_rows(key, 21, LATENTS)
    return value_matrix.astype(jnp.bfloat16)


def drawn_cross(key, salt):
    weight = drawn_weight(key, salt, (D, D))
    return weight.astype(jnp.bfloat16)


def draw_cross_query(key, part):
    return drawn_cross(key, 31)


def draw_cross_key(key, part):
    return drawn_cross(key, 32)


def draw_layer_qkv(key, part):
    weight = drawn_weight(key, 33, (LAYERS, D, 3 * D))
    return weight.astype(jnp.bfloat16)


def place_ends(entries, own_key, low, largest):
    shape = entries.shape
    spot = [jax.random.randint(jax.random.fold_in(own_key, axis), (), 0, shape[axis]) for axis in range(len(shape))]
    entries = entries.at[tuple(spot)].set(low)
    longest = shape.index(max(shape))
    spot[longest] = (spot[longest] + 1) % shape[longest]
    return entries.at[tuple(spot)].set(largest)


def steps_of(own_key, extent, cuts, smallest, largest):
    def one(position, blocks):
        steps = jax.random.uniform(jax.random.fold_in(jax.random.fold_in(own_key, 6), position), (blocks,), jnp.float32, smallest / len(cuts), largest / len(cuts))
        return jnp.repeat(jnp.exp(steps), extent[position] // blocks).reshape((-1,) + (1,) * (len(extent) - position - 1))

    factor_of = one(*cuts[0])
    for cut in cuts[1:]:
        factor_of = factor_of * one(*cut)
    return factor_of


def scatter_about(rng, extent, scale, most, split=(), held_as=jnp.bfloat16):
    values = jax.random.normal(rng, extent, jnp.float32) * scale
    if len(split) > 0:
        values = steps_of(rng, extent, split, -0.22, 0.18) * values
    return jnp.clip(values, min=-most, max=most).astype(held_as)


def setup_inputs(seed: int = 0) -> dict:
    streams_of = jax.random.split(jax.random.key(seed), 13)
    context = draw_context(jax.random.fold_in(streams_of[12], 71), 0)
    latents = draw_latents(jax.random.fold_in(streams_of[12], 71), 0)
    offsets = place_ends(jax.random.randint(streams_of[2], (B,), 0, CTX_DEV * N_SEQ - LATENTS + 1), jax.random.fold_in(streams_of[2], 1), 0, CTX_DEV * N_SEQ - LATENTS).astype(jnp.int32)
    query_gain = jnp.clip(1.0 + 0.18 * jax.random.normal(streams_of[3], (D,), jnp.float32), 0.1, 1.9)
    key_gain = jnp.clip(1.0 + 0.18 * jax.random.normal(streams_of[4], (D,), jnp.float32), 0.1, 1.9)
    layer_gain = jnp.clip(1.0 + 0.18 * jax.random.normal(streams_of[5], (LAYERS, D), jnp.float32), 0.1, 1.9)
    cross_query = draw_cross_query(jax.random.fold_in(streams_of[12], 71), 0)
    cross_key = draw_cross_key(jax.random.fold_in(streams_of[12], 71), 0)
    cross_value = scatter_about(streams_of[8], (D, D), D ** -0.5, 0.1875, ((0, 128),))
    cross_out = scatter_about(streams_of[9], (D, D), D ** -0.5, 0.1875, ((0, 128),))
    layer_qkv = draw_layer_qkv(jax.random.fold_in(streams_of[12], 71), 0)
    layer_out = scatter_about(streams_of[11], (LAYERS, D, D), D ** -0.5, 0.1875, ((1, 128),))
    return dict(context=context, latents=latents, offsets=offsets, query_gain=query_gain, key_gain=key_gain, layer_gain=layer_gain, cross_query=cross_query, cross_key=cross_key, cross_value=cross_value, cross_out=cross_out, layer_qkv=layer_qkv, layer_out=layer_out)


EPSILON = 1e-06

def rms_norm(value_matrix, gain):
    value_matrix = value_matrix.astype(jnp.float32)
    scale = lax.rsqrt(lax.optimization_barrier(jnp.mean(value_matrix * value_matrix, axis=-1, keepdims=True)) + EPSILON)
    return (value_matrix * scale * gain).astype(jnp.bfloat16)

def matmul_rows(left, weight):
    flat = left.reshape(-1, left.shape[-1])
    product = jnp.dot(flat, weight, preferred_element_type=jnp.float32)
    return product.reshape(left.shape[:-1] + (weight.shape[1],))

def cross_row(operands):
    query_matrix, key_matrix, value_matrix, offset = operands
    head_width = D // H
    count = query_matrix.shape[0]
    length = key_matrix.shape[0]
    query_head_rows = query_matrix.reshape(count, H, head_width).astype(jnp.float32)
    key_head_rows = key_matrix.reshape(length, H, head_width).astype(jnp.float32)
    value_head_rows = value_matrix.reshape(length, H, head_width).astype(jnp.float32)
    score_matrix = jnp.einsum('oqi,cqi->qoc', query_head_rows, key_head_rows) * head_width ** (-0.5)
    key_pos = jnp.arange(length, dtype=jnp.int32)
    query_pos = offset + jnp.arange(count, dtype=jnp.int32)
    valid = key_pos[None, None, :] <= query_pos[None, :, None]
    top = lax.optimization_barrier(jnp.max(jnp.where(valid, score_matrix, -1e+30), axis=2, keepdims=True))
    probability_rows = jnp.where(valid, jnp.exp(score_matrix - top), 0.0).astype(jnp.bfloat16)
    denom = lax.optimization_barrier(jnp.sum(probability_rows.astype(jnp.float32), axis=2))
    numerator_sum = jnp.einsum('ycv,vys->cys', probability_rows.astype(jnp.float32), value_head_rows)
    return (numerator_sum / jnp.transpose(denom)[:, :, None]).reshape(count, D).astype(jnp.bfloat16)

def self_row(qkv):
    head_width = D // H
    count = qkv.shape[0]
    grouped = qkv.reshape(count, 3, H, head_width).astype(jnp.float32)
    query_matrix = grouped[:, 0]
    key_matrix = grouped[:, 1]
    value_matrix = grouped[:, 2]
    score_matrix = jnp.einsum('oqi,cqi->qoc', query_matrix, key_matrix) * head_width ** (-0.5)
    positions = jnp.arange(count, dtype=jnp.int32)
    valid = positions[None, None, :] <= positions[None, :, None]
    top = lax.optimization_barrier(jnp.max(jnp.where(valid, score_matrix, -1e+30), axis=2, keepdims=True))
    probability_rows = jnp.where(valid, jnp.exp(score_matrix - top), 0.0).astype(jnp.bfloat16)
    denom = lax.optimization_barrier(jnp.sum(probability_rows.astype(jnp.float32), axis=2))
    numerator_sum = jnp.einsum('ycv,vys->cys', probability_rows.astype(jnp.float32), value_matrix)
    return (numerator_sum / jnp.transpose(denom)[:, :, None]).reshape(count, D).astype(jnp.bfloat16)

def reference(context, latents, offsets, query_gain, key_gain, layer_gain, cross_query, cross_key, cross_value, cross_out, layer_qkv, layer_out):
    normed_latents = rms_norm(latents, query_gain)
    query_matrix = matmul_rows(normed_latents, cross_query).astype(jnp.bfloat16)
    normed_context = rms_norm(context, key_gain)
    key_matrix = matmul_rows(normed_context, cross_key).astype(jnp.bfloat16)
    value_matrix = matmul_rows(normed_context, cross_value).astype(jnp.bfloat16)
    attended = lax.map(cross_row, (query_matrix, key_matrix, value_matrix, offsets.astype(jnp.int32)))
    hidden = (latents.astype(jnp.float32) + matmul_rows(attended, cross_out)).astype(jnp.bfloat16)
    for layer in range(LAYERS):
        normed = rms_norm(hidden, layer_gain[layer])
        qkv = matmul_rows(normed, layer_qkv[layer]).astype(jnp.bfloat16)
        mixed = lax.map(self_row, qkv)
        hidden = (hidden.astype(jnp.float32) + matmul_rows(mixed, layer_out[layer])).astype(jnp.bfloat16)
    return hidden
```

```python
import functools

import jax
import jax.numpy as jnp
from jax import lax
from jax.experimental import pallas as pl
from jax.experimental.pallas import tpu as pltpu
from jax.sharding import PartitionSpec as P

H = 16
EPSILON = 1e-06
NEGATIVE = -1e30
BF = jnp.bfloat16
F32 = jnp.float32
MESH = pl.DeviceIdType.MESH
N = 16
D = 1024


def normed_rows(x, gain):
    x = x.astype(F32)
    scale = lax.rsqrt(jnp.mean(x * x, axis=-1, keepdims=True) + EPSILON)
    return (x * scale * gain).astype(BF)


def dot(a, b):
    return jnp.dot(a, b, preferred_element_type=F32)


def dot_t(a, b):
    return lax.dot_general(a, b, (((1,), (1,)), ((), ())), preferred_element_type=F32)


def lanes(rows, width=128):
    return lax.broadcasted_iota(jnp.int32, (rows, width), 1)


def greet(me):
    barrier = pltpu.get_barrier_semaphore()

    @pl.loop(1, N)
    def _(d):
        pl.semaphore_signal(
            barrier, inc=1, device_id={"seq": lax.rem(me + d, N)}, device_id_type=MESH
        )


def greeted():
    pl.semaphore_wait(pltpu.get_barrier_semaphore(), N - 1)


def push(me, d, src, dst, send_sem, recv_sem):
    return pltpu.make_async_remote_copy(
        src_ref=src,
        dst_ref=dst,
        send_sem=send_sem,
        recv_sem=recv_sem,
        device_id={"seq": lax.rem(me + d, N)},
        device_id_type=MESH,
    )


def cross_kernel(
    off_ref, ctx_any, lat_any, qg_ref, kg_ref, w_any, out_ref,
    ctx, lat, w, cn, ln, keys, vals, queries, bias, part, stat, got, gstat, acc, den,
    load_sem, send_sem, recv_sem, ssend_sem, srecv_sem,
):
    me = lax.axis_index("seq")
    greet(me)
    loads = [
        pltpu.make_async_copy(ctx_any, ctx, load_sem.at[0]),
        pltpu.make_async_copy(w_any.at[:, pl.ds(D, 2 * D)], w.at[:, pl.ds(D, 2 * D)], load_sem.at[1]),
        pltpu.make_async_copy(lat_any, lat, load_sem.at[2]),
        pltpu.make_async_copy(w_any.at[:, pl.ds(0, D)], w.at[:, pl.ds(0, D)], load_sem.at[3]),
    ]
    for c in loads:
        c.start()
    C = ctx.shape[0]
    M = lat.shape[0]
    R = M // N
    S = 128
    edge = me * C - off_ref[0]
    loads[0].wait()

    @pl.loop(0, C // S)
    def _(r):
        rows = pl.ds(pl.multiple_of(r * S, S), S)
        cn[rows] = normed_rows(ctx[rows], kg_ref[...])

    loads[2].wait()

    @pl.loop(0, M // S)
    def _(r):
        rows = pl.ds(pl.multiple_of(r * S, S), S)
        ln[rows] = normed_rows(lat[rows], qg_ref[...])
        i = lax.broadcasted_iota(jnp.int32, (S, C), 0) + r * S
        j = lax.broadcasted_iota(jnp.int32, (S, C), 1)
        bias[rows] = jnp.where(j + edge <= i, 0.0, NEGATIVE)

    stat[...] = jnp.zeros_like(stat)
    loads[1].wait()

    @pl.loop(0, D // 256)
    def _(n):
        kc = pl.ds(pl.multiple_of(D + n * 256, 256), 256)
        vc = pl.ds(pl.multiple_of(2 * D + n * 256, 256), 256)
        k = dot(cn[...], w[:, kc]).astype(BF)
        keys[2 * n] = k[:, :128]
        keys[2 * n + 1] = k[:, 128:]
        v = dot(cn[...], w[:, vc]).astype(BF)
        for t in range(2):
            vals[2 * n + t, :, 0:128] = v[:, 128 * t : 128 * t + 128]
            vals[2 * n + t, :, 128:256] = jnp.ones((C, 128), BF)

    loads[3].wait()

    @pl.loop(0, D // 256)
    def _(n):
        qc = pl.ds(pl.multiple_of(n * 256, 256), 256)

        @pl.loop(0, 2)
        def _(m):
            rows = pl.ds(pl.multiple_of(m * (M // 2), M // 2), M // 2)
            q = dot(ln[rows], w[:, qc]).astype(BF) * 0.125
            queries[2 * n, rows] = q[:, :128]
            queries[2 * n + 1, rows] = q[:, 128:]

    greeted()
    T = 128

    @pl.loop(0, H // 2)
    def _(p):
        @pl.loop(0, M // T)
        def _(r):
            rows = pl.ds(pl.multiple_of(r * T, T), T)
            q = queries[p, rows]
            low = lanes(T) < 64
            outs = []
            st = stat[rows]
            for t in range(2):
                qt = jnp.where(low if t == 0 else ~low, q, jnp.zeros_like(q))
                s = dot_t(qt, keys[p]) + bias[rows]
                top = jnp.max(s, axis=1, keepdims=True)
                e = jnp.exp(s - top).astype(BF)
                o = dot(e, vals[p])
                total = o[:, 128:256]
                outs.append(o[:, 0:128] / total)
                st = jnp.where(lanes(T) == 2 * p + t, top + jnp.log(total), st)
            part[p, rows] = jnp.where(low, outs[0], outs[1]).astype(BF)
            stat[rows] = st

        @pl.loop(1, N)
        def _(d):
            there = pl.ds(pl.multiple_of(lax.rem(me + d, N) * R, R), R)
            push(me, d, part.at[p, there], got.at[d - 1, p], send_sem, recv_sem.at[d - 1]).start()

    @pl.loop(1, N)
    def _(d):
        there = pl.ds(pl.multiple_of(lax.rem(me + d, N) * R, R), R)
        push(me, d, stat.at[there], gstat.at[d - 1], ssend_sem, srecv_sem).start()

    own = pl.ds(pl.multiple_of(me * R, R), R)
    push(me, 1, gstat, gstat, ssend_sem, srecv_sem).wait_recv()
    top = stat[own]
    for d in range(N - 1):
        top = jnp.maximum(top, gstat[d])
    spread = (
        lax.broadcasted_iota(jnp.int32, (128, D), 1) // 64
        == lax.broadcasted_iota(jnp.int32, (128, D), 0)
    ).astype(F32).astype(BF)
    weight = dot(jnp.exp(stat[own] - top).astype(BF), spread)
    den[...] = weight
    for p in range(H // 2):
        cols = slice(128 * p, 128 * p + 128)
        acc[:, cols] = weight[:, cols] * part[p, own].astype(F32)

    @pl.loop(0, N - 1)
    def _(d):
        push(me, 1, got.at[d], got.at[d], send_sem, recv_sem.at[d]).wait_recv()
        weight = dot(jnp.exp(gstat[d] - top).astype(BF), spread)
        den[...] += weight
        for p in range(H // 2):
            cols = slice(128 * p, 128 * p + 128)
            acc[:, cols] += weight[:, cols] * got[d, p].astype(F32)

    out_ref[...] = (acc[...] / den[...]).astype(BF)
    push(me, 1, got, got, send_sem, recv_sem.at[0]).wait_send()
    push(me, 1, gstat, gstat, ssend_sem, srecv_sem).wait_send()


def layer_kernel(
    first, x_ref, y_ref, g_ref, w_any, out_ref,
    w, qkv, qk_out, v_out, qk_in, v_in, m_out, m_in, hid, merged,
    load_sem, send_sem, recv_sem,
):
    me = lax.axis_index("seq")
    greet(me)
    R = x_ref.shape[0]
    M = R * N
    base = D if first else 0
    loads = []
    cuts = ([(0, D)] if first else []) + [(base, 3 * D), (base + 3 * D, D)]
    for k, (start, size) in enumerate(cuts):
        cols = pl.ds(start, size)
        loads.append(pltpu.make_async_copy(w_any.at[:, cols], w.at[:, cols], load_sem.at[k]))
        loads[-1].start()
    if first:
        loads[0].wait()
        hidden = x_ref[...].astype(F32) + dot(y_ref[...], w[:, 0:D])
        hidden = hidden.astype(BF)
    else:
        hidden = x_ref[...]
    hid[...] = hidden
    normed = normed_rows(hidden, g_ref[...])
    loads[-2].wait()
    low = lanes(R) < 64
    half = R // 2

    def roll(a):
        return pltpu.roll(a.astype(F32), 64, 1).astype(BF)

    @pl.loop(0, 3 * D // 512)
    def _(n):
        cols = pl.ds(pl.multiple_of(n * 512, 512), 512)
        wide = pl.ds(pl.multiple_of(base + n * 512, 512), 512)
        qkv[:, cols] = dot(normed, w[:, wide]).astype(BF)

    lo = lanes(half) < 64
    for p in range(H // 2):
        q = qkv[:, 128 * p : 128 * p + 128] * 0.125
        k = qkv[:, D + 128 * p : D + 128 * p + 128]
        v = qkv[:, 2 * D + 128 * p : 2 * D + 128 * p + 128]
        qk_out[2 * p] = jnp.where(low, q, roll(k))
        qk_out[2 * p + 1] = jnp.where(low, roll(q), k)
        vr = roll(v)
        v_out[2 * p] = jnp.where(lo, v[:half], vr[half:])
        v_out[2 * p + 1] = jnp.where(lo, vr[:half], v[half:])
    greeted()

    @pl.loop(1, N)
    def _(d):
        to = lax.rem(me + d, N)
        push(me, d, qk_out.at[to], qk_in.at[me], send_sem.at[0], recv_sem.at[0]).start()
        push(me, d, v_out.at[to], v_in.at[me], send_sem.at[1], recv_sem.at[1]).start()

    qk_in[me] = qk_out[me]
    v_in[me] = v_out[me]
    rest = pl.ds(0, N - 1)
    push(me, 1, qk_in.at[rest], qk_in.at[rest], send_sem.at[0], recv_sem.at[0]).wait_recv()
    push(me, 1, v_in.at[rest], v_in.at[rest], send_sem.at[1], recv_sem.at[1]).wait_recv()

    qk = qk_in[...].reshape(M, 128)
    low_m = lanes(M) < 64
    kk = roll(qk)
    vp = v_in[...]
    vr = roll(vp.reshape(M // 2, 128)).reshape(N, half, 128)
    both = jnp.concatenate([vp, vr], axis=1).reshape(M, 128)
    vv = jnp.where(low_m, both, jnp.ones_like(both))
    T = 128
    for r in range(M // T):
        size = (r + 1) * T
        q = qk[r * T : size]
        q = jnp.where(lanes(T) < 64, q, jnp.zeros_like(q))
        s = dot_t(q, kk[:size])
        i = lax.broadcasted_iota(jnp.int32, (T, size), 0) + r * T
        j = lax.broadcasted_iota(jnp.int32, (T, size), 1)
        s = jnp.where(j <= i, s, NEGATIVE)
        top = jnp.max(s, axis=1, keepdims=True)
        e = jnp.exp(s - top).astype(BF)
        o = dot(e, vv[:size])
        mixed = o / pltpu.roll(o, 64, 1)
        other = pltpu.roll(mixed, 64, 1)
        for t in range(T // R):
            m_out[r * (T // R) + t] = jnp.where(
                lo, mixed[t * R : t * R + half], other[t * R + half : t * R + R]
            ).astype(BF)

    @pl.loop(1, N)
    def _(d):
        to = lax.rem(me + d, N)
        push(me, d, m_out.at[to], m_in.at[me], send_sem.at[2], recv_sem.at[2]).start()

    m_in[me] = m_out[me]
    push(me, 1, m_in.at[rest], m_in.at[rest], send_sem.at[2], recv_sem.at[2]).wait_recv()
    for p in range(H // 2):
        a = m_in[2 * p]
        b = m_in[2 * p + 1]
        merged[0:half, 128 * p : 128 * p + 128] = jnp.where(lo, a, roll(b))
        merged[half:R, 128 * p : 128 * p + 128] = jnp.where(lo, roll(a), b)
    loads[-1].wait()
    update = dot(merged[...], w[:, base + 3 * D : base + 4 * D])
    out_ref[...] = (hid[...].astype(F32) + update).astype(BF)
    push(me, 1, qk_in.at[rest], qk_in.at[rest], send_sem.at[0], recv_sem.at[0]).wait_send()
    push(me, 1, v_in.at[rest], v_in.at[rest], send_sem.at[1], recv_sem.at[1]).wait_send()
    push(me, 1, m_in.at[rest], m_in.at[rest], send_sem.at[2], recv_sem.at[2]).wait_send()


VM = pl.BlockSpec(memory_space=pltpu.VMEM)
SM = pl.BlockSpec(memory_space=pltpu.SMEM)
ANY = pl.BlockSpec(memory_space=pl.ANY)
DMA = pltpu.SemaphoreType.DMA


def params(which):
    return pltpu.CompilerParams(
        collective_id=which, has_side_effects=True, vmem_limit_bytes=48 << 20
    )


def cross(context, latents, offsets, query_gain, key_gain, weights):
    C, M = context.shape[0], latents.shape[0]
    R = M // N
    return pl.pallas_call(
        cross_kernel,
        out_shape=jax.ShapeDtypeStruct((R, D), BF),
        in_specs=[SM, ANY, ANY, VM, VM, ANY],
        out_specs=VM,
        scratch_shapes=[
            pltpu.VMEM((C, D), BF),
            pltpu.VMEM((M, D), BF),
            pltpu.VMEM((D, 3 * D), BF),
            pltpu.VMEM((C, D), BF),
            pltpu.VMEM((M, D), BF),
            pltpu.VMEM((H // 2, C, 128), BF),
            pltpu.VMEM((H // 2, C, 256), BF),
            pltpu.VMEM((H // 2, M, 128), BF),
            pltpu.VMEM((M, C), F32),
            pltpu.VMEM((H // 2, M, 128), BF),
            pltpu.VMEM((M, 128), F32),
            pltpu.VMEM((N - 1, H // 2, R, 128), BF),
            pltpu.VMEM((N - 1, R, 128), F32),
            pltpu.VMEM((R, D), F32),
            pltpu.VMEM((R, D), F32),
            DMA((4,)),
            DMA,
            DMA((N - 1,)),
            DMA,
            DMA,
        ],
        compiler_params=params(0),
        cost_estimate=pl.CostEstimate(
            flops=30 * 10**9, bytes_accessed=10 << 20, transcendentals=8 << 20
        ),
        name="cross",
    )(offsets, context, latents, query_gain, key_gain, weights)


def layer(which, hidden, attended, gain, weights):
    R = hidden.shape[0]
    first = which == 1
    return pl.pallas_call(
        functools.partial(layer_kernel, first),
        out_shape=jax.ShapeDtypeStruct((R, D), BF),
        in_specs=[VM, VM, VM, ANY],
        out_specs=VM,
        scratch_shapes=[
            pltpu.VMEM(weights.shape, BF),
            pltpu.VMEM((R, 3 * D), BF),
            pltpu.VMEM((H, R, 128), BF),
            pltpu.VMEM((H, R // 2, 128), BF),
            pltpu.VMEM((N, R, 128), BF),
            pltpu.VMEM((N, R // 2, 128), BF),
            pltpu.VMEM((N, R // 2, 128), BF),
            pltpu.VMEM((H, R // 2, 128), BF),
            pltpu.VMEM((R, D), BF),
            pltpu.VMEM((R, D), BF),
            DMA((3,)),
            DMA((3,)),
            DMA((3,)),
        ],
        compiler_params=params(which),
        cost_estimate=pl.CostEstimate(
            flops=10 * 10**9, bytes_accessed=10 << 20, transcendentals=1 << 20
        ),
        name=f"layer{which}",
    )(hidden, attended, gain, weights)


def per_device(
    context,
    latents,
    offsets,
    query_gain,
    key_gain,
    layer_gain,
    cross_query,
    cross_key,
    cross_value,
    cross_out,
    layer_qkv,
    layer_out,
):
    def gather(*pieces):
        return lax.all_gather(
            jnp.concatenate(pieces, axis=1), ("seq", "head"), axis=0, tiled=True
        )

    M = latents.shape[1]
    R = M // N
    w0 = gather(cross_query, cross_key, cross_value)
    w1 = gather(cross_out, layer_qkv[0], layer_out[0])
    w2 = gather(layer_qkv[1], layer_out[1])
    own = lax.dynamic_slice_in_dim(latents[0], lax.axis_index("seq") * R, R, 0)
    attended = cross(
        context[0], latents[0], offsets, query_gain[None], key_gain[None], w0
    )
    hidden = layer(1, own, attended, layer_gain[0:1], w1)
    hidden = layer(2, hidden, hidden, layer_gain[1:2], w2)
    return hidden[None]


def solution(mesh):
    return jax.shard_map(
        per_device,
        mesh=mesh,
        in_specs=(
            P("head", "seq", None),
            P("head", None, None),
            P("head"),
            P(),
            P(),
            P(),
            P(("seq", "head"), None),
            P(("seq", "head"), None),
            P(("seq", "head"), None),
            P(("seq", "head"), None),
            P(None, ("seq", "head"), None),
            P(None, ("seq", "head"), None),
        ),
        out_specs=P("head", "seq", None),
        check_vma=False,
    )
```

```python
import functools

import jax
import jax.numpy as jnp
from jax import lax
from jax.experimental import pallas as pl
from jax.experimental.pallas import tpu as pltpu
from jax.sharding import PartitionSpec as P

H = 16
EPSILON = 1e-06
NEGATIVE = -1e30
BF = jnp.bfloat16
F32 = jnp.float32
MESH = pl.DeviceIdType.MESH
N = 16
D = 1024


def normed_rows(x, gain):
    x = x.astype(F32)
    scale = lax.rsqrt(jnp.mean(x * x, axis=-1, keepdims=True) + EPSILON)
    return (x * scale * gain).astype(BF)


def dot(a, b):
    return jnp.dot(a, b, preferred_element_type=F32)


def dot_t(a, b):
    return lax.dot_general(a, b, (((1,), (1,)), ((), ())), preferred_element_type=F32)


def lanes(rows, width=128):
    return lax.broadcasted_iota(jnp.int32, (rows, width), 1)


K = 4
ROUNDS = ((0, 1), (3, 2), (9, 1))


class Gather:
    def __init__(self, w, blank, sems):
        self.w, self.blank = w, blank
        self.near_sem, self.side_sem, self.far_sem, self.mate_sem, self.sent_sem = sems
        me, lane = lax.axis_index("seq"), lax.axis_index("head")
        self.me = me
        self.at = (me // K, lax.rem(me, K), lane // 2)
        self.core = lax.rem(lane, 2)

    def device(self, at, core=None):
        core = self.core if core is None else core
        return {"seq": at[0] * K + at[1], "head": at[2] * 2 + core}

    def plane(self, axis):
        a, b = [i for i in range(3) if i != axis]
        flat = self.at[a] * K + self.at[b]

        def peer(i):
            j = lax.rem(flat + i, K * K)
            at = list(self.at)
            at[a], at[b] = j // K, lax.rem(j, K)
            return at

        return peer

    def along(self, axis, step):
        at = list(self.at)
        at[axis] = lax.rem(at[axis] + step, K)
        return at

    def units(self, g, axis):
        start, k = ROUNDS[g]
        return pl.ds(start + axis * k, k)

    def own(self, g, axis):
        return self.w.at[(self.units(g, axis), *self.at, self.core)]

    def slab(self, g, axis, step, half=None):
        index = [slice(None)] * 3
        index[axis] = lax.rem(self.at[axis] + step, K)
        if half is not None:
            index[1 if axis == 0 else 0] = pl.ds(2 * half, 2)
        return self.w.at[(self.units(g, axis), *index, self.core)]

    def copy(self, ref, sent, recv, device):
        return pltpu.make_async_remote_copy(
            src_ref=ref, dst_ref=ref, send_sem=sent, recv_sem=recv,
            device_id=device, device_id_type=MESH,
        )

    def wait_for(self, ref, sem):
        self.copy(ref, self.sent_sem.at[0, 0, 0], sem, self.device(self.at, 1 - self.core)).wait_recv()

    def to_mate(self, g, axis, step):
        self.copy(
            self.slab(g, axis, step), self.sent_sem.at[g, axis, 3], self.mate_sem.at[g, axis],
            self.device(self.at, 1 - self.core),
        ).start()

    def greet(self):
        barrier = pltpu.get_barrier_semaphore()
        for axis in range(3):
            peer = self.plane(axis)

            @pl.loop(1, K * K)
            def _(i):
                pl.semaphore_signal(
                    barrier, inc=1, device_id=self.device(peer(i)), device_id_type=MESH
                )

        pl.semaphore_signal(
            barrier, inc=1, device_id=self.device(self.at, 1 - self.core), device_id_type=MESH
        )
        pl.semaphore_wait(barrier, 3 * (K * K - 1) + 1)

    def begin(self, g):
        for axis in range(3):
            peer = self.plane(axis)

            @pl.loop(1, K * K)
            def _(i):
                self.copy(
                    self.own(g, axis), self.sent_sem.at[g, axis, 0], self.near_sem.at[g, axis],
                    self.device(peer(i)),
                ).start()

    def second(self, g):
        for axis in range(3):
            k = ROUNDS[g][1]
            self.wait_for(self.blank.at[pl.ds(0, (K * K - 1) * k)], self.near_sem.at[g, axis])
            for side, step in enumerate((1, 3)):
                self.copy(
                    self.slab(g, axis, 0), self.sent_sem.at[g, axis, 1],
                    self.side_sem.at[g, axis, side], self.device(self.along(axis, step)),
                ).start()
        for axis in range(3):
            self.to_mate(g, axis, 0)

    def third(self, g):
        for axis in range(3):
            for side, step in enumerate((1, 3)):
                self.wait_for(self.slab(g, axis, 4 - step), self.side_sem.at[g, axis, side])
                self.copy(
                    self.slab(g, axis, 4 - step, side), self.sent_sem.at[g, axis, 2],
                    self.far_sem.at[g, axis, side], self.device(self.along(axis, step)),
                ).start()
            self.to_mate(g, axis, 1)
            self.to_mate(g, axis, 3)

    def fourth(self, g):
        for axis in range(3):
            for side in range(2):
                self.wait_for(self.slab(g, axis, 2, side), self.far_sem.at[g, axis, side])
            self.to_mate(g, axis, 2)

    def ready(self, g, axes=(0, 1, 2)):
        for axis in axes:
            self.wait_for(
                self.w.at[(self.units(g, axis), slice(None), slice(None), slice(None), self.core)],
                self.mate_sem.at[g, axis],
            )

    def close(self):
        for g in range(len(ROUNDS)):
            k = ROUNDS[g][1]
            for axis in range(3):
                units = self.units(g, axis)
                everything = (slice(None),) * 3
                for phase, ref in enumerate((
                    self.blank.at[pl.ds(0, (K * K - 1) * k)],
                    self.w.at[(units, pl.ds(0, 2), slice(None), slice(None), self.core)],
                    self.w.at[(units, pl.ds(0, 1), slice(None), slice(None), self.core)],
                    self.w.at[(units, *everything, self.core)],
                )):
                    self.copy(
                        ref, self.sent_sem.at[g, axis, phase], self.near_sem.at[g, axis],
                        self.device(self.at, 1 - self.core),
                    ).wait_send()


def push(me, d, src, dst, send_sem, recv_sem):
    return pltpu.make_async_remote_copy(
        src_ref=src,
        dst_ref=dst,
        send_sem=send_sem,
        recv_sem=recv_sem,
        device_id={"seq": lax.rem(me + d, N)},
        device_id_type=MESH,
    )


def roll(a):
    return pltpu.roll(a.astype(F32), 64, 1).astype(BF)


KEY, VALUE, QUERY, OUT = 0, 1, 2, 3
LAYER_UNITS = ((4, 5, 6, 7), (8, 9, 10, 11))


def kernel(
    off_ref, ctx_any, lat_any, qg_any, kg_any, lg_any, cq_any, ck_any, cv_any, co_any, lq_any, lo_any,
    out_ref,
    ctx, lat, qg, kg, lg, w, blank, cn, ln, keys, vals, queries, bias, part, stat, got, gstat,
    acc, den, att, hid, norm, qkv, qk_out, v_out, qk_in, v_in, m_out, m_in, merged,
    load_sem, shard_sem, near_sem, side_sem, far_sem, mate_sem, sent_sem,
    send_sem, recv_sem, ssend_sem, srecv_sem, lsend_sem, lrecv_sem,
):
    me = lax.axis_index("seq")
    gather = Gather(w, blank, (near_sem, side_sem, far_sem, mate_sem, sent_sem))
    shards = [ck_any, cv_any, cq_any, co_any]
    for l in range(2):
        shards += [lq_any.at[l, :, pl.ds(D * t, D)] for t in range(3)] + [lo_any.at[l]]
    shards = [
        pltpu.make_async_copy(s, w.at[(u, *gather.at, gather.core)], shard_sem.at[u])
        for u, s in enumerate(shards)
    ]
    loads = [
        pltpu.make_async_copy(a, b, load_sem.at[i])
        for i, (a, b) in enumerate((
            (kg_any, kg), (ctx_any.at[0], ctx), (qg_any, qg), (lat_any.at[0], lat), (lg_any, lg),
        ))
    ]
    for c in shards[:3] + loads + shards[3:]:
        c.start()
    gather.greet()
    for c in shards[:3]:
        c.wait()
    gather.begin(0)
    C = ctx.shape[0]
    M = lat.shape[0]
    R = M // N
    S = 128
    edge = me * C - off_ref[0]
    loads[0].wait()
    loads[1].wait()

    @pl.loop(0, C // S)
    def _(r):
        rows = pl.ds(pl.multiple_of(r * S, S), S)
        cn[rows] = normed_rows(ctx[rows], kg[...])

    stat[...] = jnp.zeros_like(stat)
    gather.second(0)
    for c in shards[3:]:
        c.wait()
    gather.begin(1)
    loads[2].wait()
    loads[3].wait()
    loads[4].wait()

    @pl.loop(0, M // S)
    def _(r):
        rows = pl.ds(pl.multiple_of(r * S, S), S)
        ln[rows] = normed_rows(lat[rows], qg[...])
        i = lax.broadcasted_iota(jnp.int32, (S, C), 0) + r * S
        j = lax.broadcasted_iota(jnp.int32, (S, C), 1)
        bias[rows] = jnp.where(j + edge <= i, 0.0, NEGATIVE)

    gather.third(0)
    gather.fourth(0)
    gather.second(1)
    gather.ready(0)

    def unit(u, cols):
        return w[u, :, :, :, :, :, cols].reshape(D, -1)

    @pl.loop(0, D // 256)
    def _(n):
        cols = pl.ds(pl.multiple_of(n * 256, 256), 256)
        k = dot(cn[...], unit(KEY, cols)).astype(BF)
        keys[2 * n] = k[:, :128]
        keys[2 * n + 1] = k[:, 128:]
        v = dot(cn[...], unit(VALUE, cols)).astype(BF)
        for t in range(2):
            vals[2 * n + t, :, 0:128] = v[:, 128 * t : 128 * t + 128]
            vals[2 * n + t, :, 128:256] = jnp.ones((C, 128), BF)

        @pl.loop(0, 2)
        def _(m):
            rows = pl.ds(pl.multiple_of(m * (M // 2), M // 2), M // 2)
            q = dot(ln[rows], unit(QUERY, cols)).astype(BF) * 0.125
            queries[2 * n, rows] = q[:, :128]
            queries[2 * n + 1, rows] = q[:, 128:]

    T = 128

    @pl.loop(0, H // 2)
    def _(p):
        @pl.loop(0, M // T)
        def _(r):
            rows = pl.ds(pl.multiple_of(r * T, T), T)
            q = queries[p, rows]
            low = lanes(T) < 64
            outs = []
            st = stat[rows]
            for t in range(2):
                qt = jnp.where(low if t == 0 else ~low, q, jnp.zeros_like(q))
                s = dot_t(qt, keys[p]) + bias[rows]
                top = jnp.max(s, axis=1, keepdims=True)
                e = jnp.exp(s - top).astype(BF)
                o = dot(e, vals[p])
                total = o[:, 128:256]
                outs.append(o[:, 0:128] / total)
                st = jnp.where(lanes(T) == 2 * p + t, top + jnp.log(total), st)
            part[p, rows] = jnp.where(low, outs[0], outs[1]).astype(BF)
            stat[rows] = st

        @pl.loop(1, N)
        def _(d):
            there = pl.ds(pl.multiple_of(lax.rem(me + d, N) * R, R), R)
            push(me, d, part.at[p, there], got.at[d - 1, p], send_sem, recv_sem.at[d - 1]).start()

        @pl.when(p == 1)
        def _():
            gather.third(1)
            gather.begin(2)

        @pl.when(p == 4)
        def _():
            gather.fourth(1)
            gather.second(2)

    @pl.loop(1, N)
    def _(d):
        there = pl.ds(pl.multiple_of(lax.rem(me + d, N) * R, R), R)
        push(me, d, stat.at[there], gstat.at[d - 1], ssend_sem, srecv_sem).start()

    gather.third(2)
    own = pl.ds(pl.multiple_of(me * R, R), R)
    push(me, 1, gstat, gstat, ssend_sem, srecv_sem).wait_recv()
    top = stat[own]
    for d in range(N - 1):
        top = jnp.maximum(top, gstat[d])
    spread = (
        lax.broadcasted_iota(jnp.int32, (128, D), 1) // 64
        == lax.broadcasted_iota(jnp.int32, (128, D), 0)
    ).astype(F32).astype(BF)
    weight = dot(jnp.exp(stat[own] - top).astype(BF), spread)
    den[...] = weight
    for p in range(H // 2):
        cols = slice(128 * p, 128 * p + 128)
        acc[:, cols] = weight[:, cols] * part[p, own].astype(F32)

    @pl.loop(0, N - 1)
    def _(d):
        push(me, 1, got.at[d], got.at[d], send_sem, recv_sem.at[d]).wait_recv()
        weight = dot(jnp.exp(gstat[d] - top).astype(BF), spread)
        den[...] += weight
        for p in range(H // 2):
            cols = slice(128 * p, 128 * p + 128)
            acc[:, cols] += weight[:, cols] * got[d, p].astype(F32)

    att[...] = (acc[...] / den[...]).astype(BF)
    gather.ready(1)
    hid[...] = lat[own]

    def add_update(rows_ref, u):
        @pl.loop(0, D // 256)
        def _(n):
            cols = pl.ds(pl.multiple_of(n * 256, 256), 256)
            update = dot(rows_ref[...], unit(u, cols))
            hid[:, cols] = (hid[:, cols].astype(F32) + update).astype(BF)

    add_update(att, OUT)
    low = lanes(R) < 64
    half = R // 2
    lo = lanes(half) < 64
    rest = pl.ds(0, N - 1)

    def exchange(l, t, src, dst, start):
        if start:
            @pl.loop(1, N)
            def _(d):
                to = lax.rem(me + d, N)
                push(me, d, src.at[to], dst.at[l, me], lsend_sem.at[l, t], lrecv_sem.at[l, t]).start()

            dst[l, me] = src[me]
        return push(me, 1, dst.at[l, rest], dst.at[l, rest], lsend_sem.at[l, t], lrecv_sem.at[l, t])

    for l in range(2):
        units = LAYER_UNITS[l]
        if l == 1:
            gather.ready(2)
        norm[...] = normed_rows(hid[...], lg[l : l + 1])
        for t in range(3):
            @pl.loop(0, D // 256)
            def _(n):
                cols = pl.ds(pl.multiple_of(n * 256, 256), 256)
                qkv[:, pl.ds(pl.multiple_of(D * t + n * 256, 256), 256)] = dot(
                    norm[...], unit(units[t], cols)
                ).astype(BF)

        if l == 1:
            exchange(0, 0, qk_out, qk_in, False).wait_send()
            exchange(0, 1, v_out, v_in, False).wait_send()
            exchange(0, 2, m_out, m_in, False).wait_send()
        for p in range(H // 2):
            q = qkv[:, 128 * p : 128 * p + 128] * 0.125
            k = qkv[:, D + 128 * p : D + 128 * p + 128]
            v = qkv[:, 2 * D + 128 * p : 2 * D + 128 * p + 128]
            qk_out[2 * p] = jnp.where(low, q, roll(k))
            qk_out[2 * p + 1] = jnp.where(low, roll(q), k)
            vr = roll(v)
            v_out[2 * p] = jnp.where(lo, v[:half], vr[half:])
            v_out[2 * p + 1] = jnp.where(lo, vr[:half], v[half:])
        exchange(l, 0, qk_out, qk_in, True)
        exchange(l, 1, v_out, v_in, True)
        if l == 0:
            gather.fourth(2)
        exchange(l, 0, qk_out, qk_in, False).wait_recv()
        exchange(l, 1, v_out, v_in, False).wait_recv()

        qk = qk_in[l].reshape(M, 128)
        kk = roll(qk)
        vp = v_in[l]
        vr = roll(vp.reshape(M // 2, 128)).reshape(N, half, 128)
        both = jnp.concatenate([vp, vr], axis=1).reshape(M, 128)
        vv = jnp.where(lanes(M) < 64, both, jnp.ones_like(both))
        for r in range(M // T):
            size = (r + 1) * T
            q = qk[r * T : size]
            q = jnp.where(lanes(T) < 64, q, jnp.zeros_like(q))
            s = dot_t(q, kk[:size])
            i = lax.broadcasted_iota(jnp.int32, (T, size), 0) + r * T
            j = lax.broadcasted_iota(jnp.int32, (T, size), 1)
            s = jnp.where(j <= i, s, NEGATIVE)
            top = jnp.max(s, axis=1, keepdims=True)
            e = jnp.exp(s - top).astype(BF)
            o = dot(e, vv[:size])
            mixed = o / pltpu.roll(o, 64, 1)
            other = pltpu.roll(mixed, 64, 1)
            for t in range(T // R):
                m_out[r * (T // R) + t] = jnp.where(
                    lo, mixed[t * R : t * R + half], other[t * R + half : t * R + R]
                ).astype(BF)

        exchange(l, 2, m_out, m_in, True)
        exchange(l, 2, m_out, m_in, False).wait_recv()
        for p in range(H // 2):
            a = m_in[l, 2 * p]
            b = m_in[l, 2 * p + 1]
            merged[0:half, 128 * p : 128 * p + 128] = jnp.where(lo, a, roll(b))
            merged[half:R, 128 * p : 128 * p + 128] = jnp.where(lo, roll(a), b)
        add_update(merged, units[3])

    out_ref[0] = hid[...]
    push(me, 1, got, got, send_sem, recv_sem.at[0]).wait_send()
    push(me, 1, gstat, gstat, ssend_sem, srecv_sem).wait_send()
    exchange(1, 0, qk_out, qk_in, False).wait_send()
    exchange(1, 1, v_out, v_in, False).wait_send()
    exchange(1, 2, m_out, m_in, False).wait_send()
    gather.close()


VM = pl.BlockSpec(memory_space=pltpu.VMEM)
SM = pl.BlockSpec(memory_space=pltpu.SMEM)
ANY = pl.BlockSpec(memory_space=pl.ANY)
DMA = pltpu.SemaphoreType.DMA


def per_device(
    context,
    latents,
    offsets,
    query_gain,
    key_gain,
    layer_gain,
    cross_query,
    cross_key,
    cross_value,
    cross_out,
    layer_qkv,
    layer_out,
):
    C, M = context.shape[1], latents.shape[1]
    R = M // N
    G = len(ROUNDS)
    most = max(k for _, k in ROUNDS)
    return pl.pallas_call(
        kernel,
        out_shape=jax.ShapeDtypeStruct((1, R, D), BF),
        in_specs=[SM] + [ANY] * 11,
        out_specs=VM,
        scratch_shapes=[
            pltpu.VMEM((C, D), BF),
            pltpu.VMEM((M, D), BF),
            pltpu.VMEM((1, D), F32),
            pltpu.VMEM((1, D), F32),
            pltpu.VMEM((2, D), F32),
            pltpu.VMEM((12, K, K, K, 2, 8, D), BF),
            pltpu.VMEM(((K * K - 1) * most, 8, D), BF),
            pltpu.VMEM((C, D), BF),
            pltpu.VMEM((M, D), BF),
            pltpu.VMEM((H // 2, C, 128), BF),
            pltpu.VMEM((H // 2, C, 256), BF),
            pltpu.VMEM((H // 2, M, 128), BF),
            pltpu.VMEM((M, C), F32),
            pltpu.VMEM((H // 2, M, 128), BF),
            pltpu.VMEM((M, 128), F32),
            pltpu.VMEM((N - 1, H // 2, R, 128), BF),
            pltpu.VMEM((N - 1, R, 128), F32),
            pltpu.VMEM((R, D), F32),
            pltpu.VMEM((R, D), F32),
            pltpu.VMEM((R, D), BF),
            pltpu.VMEM((R, D), BF),
            pltpu.VMEM((R, D), BF),
            pltpu.VMEM((R, 3 * D), BF),
            pltpu.VMEM((H, R, 128), BF),
            pltpu.VMEM((H, R // 2, 128), BF),
            pltpu.VMEM((2, N, R, 128), BF),
            pltpu.VMEM((2, N, R // 2, 128), BF),
            pltpu.VMEM((N, R // 2, 128), BF),
            pltpu.VMEM((2, H, R // 2, 128), BF),
            pltpu.VMEM((R, D), BF),
            DMA((5,)),
            DMA((12,)),
            DMA((G, 3)),
            DMA((G, 3, 2)),
            DMA((G, 3, 2)),
            DMA((G, 3)),
            DMA((G, 3, 4)),
            DMA,
            DMA((N - 1,)),
            DMA,
            DMA,
            DMA((2, 3)),
            DMA((2, 3)),
        ],
        compiler_params=pltpu.CompilerParams(
            collective_id=0, has_side_effects=True, vmem_limit_bytes=60 << 20
        ),
        name="window",
    )(
        offsets, context, latents, query_gain[None], key_gain[None], layer_gain,
        cross_query, cross_key, cross_value, cross_out, layer_qkv, layer_out,
    )

def solution(mesh):
    return jax.shard_map(
        per_device,
        mesh=mesh,
        in_specs=(
            P("head", "seq", None),
            P("head", None, None),
            P("head"),
            P(),
            P(),
            P(),
            P(("seq", "head"), None),
            P(("seq", "head"), None),
            P(("seq", "head"), None),
            P(("seq", "head"), None),
            P(None, ("seq", "head"), None),
            P(None, ("seq", "head"), None),
        ),
        out_specs=P("head", "seq", None),
        check_vma=False,
    )
```

```python
import functools

import jax
import jax.numpy as jnp
from jax import lax
from jax.experimental import pallas as pl
from jax.experimental.pallas import tpu as pltpu
from jax.sharding import PartitionSpec as P

H = 16
EPSILON = 1e-06
NEGATIVE = -1e30
BF = jnp.bfloat16
F32 = jnp.float32
MESH = pl.DeviceIdType.MESH
N = 16
D = 1024


def normed_rows(x, gain):
    x = x.astype(F32)
    scale = lax.rsqrt(jnp.mean(x * x, axis=-1, keepdims=True) + EPSILON)
    return (x * scale * gain).astype(BF)


def dot(a, b):
    return jnp.dot(a, b, preferred_element_type=F32)


def dot_t(a, b):
    return lax.dot_general(a, b, (((1,), (1,)), ((), ())), preferred_element_type=F32)


def lanes(rows, width=128):
    return lax.broadcasted_iota(jnp.int32, (rows, width), 1)


K = 4
X, Z, Y = 0, 1, 2
GROUPS = (
    (0, 1, X, Y, Z, 0),
    (1, 1, Y, X, Z, 0),
    (2, 1, Z, X, Y, 0),
    (3, 1, X, Y, Z, 0),
    (4, 1, Y, X, Z, 0),
    (5, 1, Z, X, Y, 0),
    (6, 2, Y, X, Z, 1),
    (8, 2, Y, Z, X, 1),
    (10, 2, X, Y, Z, 1),
    (12, 2, Z, Y, X, 1),
    (14, 2, Y, X, Z, 1),
    (16, 2, Y, Z, X, 1),
    (18, 2, X, Y, Z, 1),
    (20, 2, Z, Y, X, 1),
    (22, 2, Y, X, Z, 1),
)


class Gather:
    def __init__(self, w, blank, sems):
        self.w, self.blank = w, blank
        self.line_sem, self.near_sem, self.side_sem, self.far_sem, self.mate_sem, self.sent_sem = sems
        me, lane = lax.axis_index("seq"), lax.axis_index("head")
        self.me = me
        self.at = (me // K, lax.rem(me, K), lane // 2)
        self.core = lax.rem(lane, 2)

    def device(self, at, core=None):
        core = self.core if core is None else core
        return {"seq": at[0] * K + at[1], "head": at[2] * 2 + core}

    def mate(self):
        return self.device(self.at, 1 - self.core)

    def plane(self, axis):
        a, b = [i for i in range(3) if i != axis]
        flat = self.at[a] * K + self.at[b]

        def peer(i):
            j = lax.rem(flat + i, K * K)
            at = list(self.at)
            at[a], at[b] = j // K, lax.rem(j, K)
            return at

        return peer

    def along(self, axis, step):
        at = list(self.at)
        at[axis] = lax.rem(at[axis] + step, K)
        return at

    def units(self, g):
        return pl.ds(GROUPS[g][0], GROUPS[g][1])

    def own(self, g):
        return self.w.at[(self.units(g), *self.at, self.core)]

    def line(self, g):
        index = list(self.at)
        index[GROUPS[g][3]] = slice(None)
        return self.w.at[(self.units(g), *index, self.core)]

    def slab(self, g, step, half=None):
        axis = GROUPS[g][2]
        index = [slice(None)] * 3
        index[axis] = lax.rem(self.at[axis] + step, K)
        if half is not None:
            index[1 if axis == 0 else 0] = pl.ds(2 * half, 2)
        return self.w.at[(self.units(g), *index, self.core)]

    def copy(self, ref, sent, recv, device):
        return pltpu.make_async_remote_copy(
            src_ref=ref, dst_ref=ref, send_sem=sent, recv_sem=recv,
            device_id=device, device_id_type=MESH,
        )

    def wait_for(self, ref, sem):
        self.copy(ref, self.sent_sem.at[0, 0], sem, self.mate()).wait_recv()

    def blanks(self, g, n):
        return self.blank.at[pl.ds(0, n * GROUPS[g][1])]

    def to_mate(self, g, step):
        self.copy(
            self.slab(g, step), self.sent_sem.at[g, 3], self.mate_sem.at[g], self.mate()
        ).start()

    def greet(self):
        barrier = pltpu.get_barrier_semaphore()
        for axis in range(3):
            peer = self.plane(axis)

            @pl.loop(1, K * K)
            def _(i):
                pl.semaphore_signal(
                    barrier, inc=1, device_id=self.device(peer(i)), device_id_type=MESH
                )

        pl.semaphore_signal(barrier, inc=1, device_id=self.mate(), device_id_type=MESH)
        pl.semaphore_wait(barrier, 3 * (K * K - 1) + 1)

    def begin(self, *groups):
        for g in groups:
            _, k, axis, first, second, steps = GROUPS[g]
            if steps:
                for i in range(1, K):
                    self.copy(
                        self.own(g), self.sent_sem.at[g, 4], self.line_sem.at[g],
                        self.device(self.along(first, i)),
                    ).start()
            else:
                peer = self.plane(axis)

                @pl.loop(1, K * K)
                def _(i):
                    self.copy(
                        self.own(g), self.sent_sem.at[g, 0], self.near_sem.at[g],
                        self.device(peer(i)),
                    ).start()

    def first(self, *groups):
        for g in groups:
            self.wait_for(self.blanks(g, K - 1), self.line_sem.at[g])
            for i in range(1, K):
                self.copy(
                    self.line(g), self.sent_sem.at[g, 0], self.near_sem.at[g],
                    self.device(self.along(GROUPS[g][4], i)),
                ).start()

    def second(self, *groups):
        for g in groups:
            n = K * (K - 1) if GROUPS[g][5] else K * K - 1
            self.wait_for(self.blanks(g, n), self.near_sem.at[g])
            for side, step in enumerate((1, 3)):
                self.copy(
                    self.slab(g, 0), self.sent_sem.at[g, 1],
                    self.side_sem.at[g, side], self.device(self.along(GROUPS[g][2], step)),
                ).start()
        for g in groups:
            self.to_mate(g, 0)

    def third(self, *groups):
        for g in groups:
            for side, step in enumerate((1, 3)):
                self.wait_for(self.slab(g, 4 - step), self.side_sem.at[g, side])
                self.copy(
                    self.slab(g, 4 - step, side), self.sent_sem.at[g, 2],
                    self.far_sem.at[g, side], self.device(self.along(GROUPS[g][2], step)),
                ).start()
        for g in groups:
            self.to_mate(g, 1)
            self.to_mate(g, 3)

    def fourth(self, *groups):
        for g in groups:
            for side in range(2):
                self.wait_for(self.slab(g, 2, side), self.far_sem.at[g, side])
            self.to_mate(g, 2)

    def ready(self, *groups):
        for g in groups:
            self.wait_for(
                self.w.at[(self.units(g), slice(None), slice(None), slice(None), self.core)],
                self.mate_sem.at[g],
            )

    def close(self):
        full = slice(None)
        for g in range(len(GROUPS)):
            units = self.units(g)
            steps = GROUPS[g][5]
            ends = [
                (0, self.blanks(g, K * (K - 1) if steps else K * K - 1)),
                (1, self.w.at[(units, pl.ds(0, 2), full, full, self.core)]),
                (2, self.w.at[(units, pl.ds(0, 1), full, full, self.core)]),
                (3, self.w.at[(units, full, full, full, self.core)]),
            ]
            if steps:
                ends.append((4, self.blanks(g, K - 1)))
            for phase, ref in ends:
                self.copy(ref, self.sent_sem.at[g, phase], self.near_sem.at[g], self.mate()).wait_send()


def push(me, d, src, dst, send_sem, recv_sem):
    return pltpu.make_async_remote_copy(
        src_ref=src,
        dst_ref=dst,
        send_sem=send_sem,
        recv_sem=recv_sem,
        device_id={"seq": lax.rem(me + d, N)},
        device_id_type=MESH,
    )


def roll(a):
    return pltpu.roll(a.astype(F32), 64, 1).astype(BF)


def folded(block):
    out = block[0:8]
    for t in range(1, 8):
        out = out + pltpu.roll(block[8 * t : 8 * t + 8], 16 * t, 1)
    return out


def unfolded(small):
    return jnp.concatenate(
        [small] + [pltpu.roll(small, 128 - 16 * t, 1) for t in range(1, 8)], axis=0
    )


KEY, VALUE, QUERY = 0, 1, 2
OUT = 6
LAYER_UNITS = ((8, 10, 12, 14), (16, 18, 20, 22))
HALF = D // 2


def kernel(
    off_ref, ctx_any, lat_any, qg_any, kg_any, lg_any, cq_any, ck_any, cv_any, co_any, lq_any, lo_any,
    out_ref,
    ctx, lat, qg, kg, lg, w, blank, cn, ln, keys, vals, queries, bias, part, stat, fold,
    got1, gf1, mid, mf, got2, gf2,
    att, hid, norm, qk_out, v_out, qk_in, v_in, m_out, m_in, merged,
    load_sem, shard_sem, line_sem, near_sem, side_sem, far_sem, mate_sem, sent_sem,
    rs_send, rs_recv, lsend_sem, lrecv_sem,
):
    me = lax.axis_index("seq")
    gather = Gather(w, blank, (line_sem, near_sem, side_sem, far_sem, mate_sem, sent_sem))
    here = gather.at
    shards = [a.at[:, pl.ds(HALF * t, HALF)] for t in range(2) for a in (ck_any, cv_any, cq_any)]
    shards += [co_any.at[:, pl.ds(HALF * t, HALF)] for t in range(2)]
    for l in range(2):
        shards += [lq_any.at[l, :, pl.ds(HALF * t, HALF)] for t in range(6)]
        shards += [lo_any.at[l, :, pl.ds(HALF * t, HALF)] for t in range(2)]
    shards = [
        pltpu.make_async_copy(s, w.at[(u, *here, gather.core)], shard_sem.at[u])
        for u, s in enumerate(shards)
    ]
    loads = [
        pltpu.make_async_copy(a, b, load_sem.at[i])
        for i, (a, b) in enumerate((
            (kg_any, kg), (ctx_any.at[0], ctx), (qg_any, qg), (lat_any.at[0], lat), (lg_any, lg),
        ))
    ]
    for c in shards[:6] + loads + shards[6:]:
        c.start()
    gather.greet()
    for c in shards[:6]:
        c.wait()
    gather.begin(0, 1, 2)
    gather.begin(3, 4, 5)
    C = ctx.shape[0]
    M = lat.shape[0]
    R = M // N
    S = 128
    edge = me * C - off_ref[0]
    loads[0].wait()
    loads[1].wait()

    @pl.loop(0, C // S)
    def _(r):
        rows = pl.ds(pl.multiple_of(r * S, S), S)
        cn[rows] = normed_rows(ctx[rows], kg[...])

    stat[...] = jnp.zeros_like(stat)
    vals[:, :, 128:256] = jnp.ones((H // 2, C, 128), BF)
    for c in loads[2:] + shards[6:]:
        c.wait()
    gather.second(0, 1, 2)

    @pl.loop(0, M // S)
    def _(r):
        rows = pl.ds(pl.multiple_of(r * S, S), S)
        ln[rows] = normed_rows(lat[rows], qg[...])
        i = lax.broadcasted_iota(jnp.int32, (S, C), 0) + r * S
        j = lax.broadcasted_iota(jnp.int32, (S, C), 1)
        bias[rows] = jnp.where(j + edge <= i, 0.0, NEGATIVE)

    early, late = (6, 7, 8, 9), (10, 11, 12, 13, 14)
    gather.second(3, 4, 5)
    gather.third(0, 1, 2)
    gather.third(3, 4, 5)
    gather.begin(*early, *late)
    gather.fourth(0, 1, 2)
    gather.first(*early)
    gather.ready(0, 1, 2)

    def piece(u, n):
        cols = pl.ds(pl.multiple_of(n * 256, 256), 256)
        return w[u, :, :, :, :, :, cols].reshape(D, 256)

    def unit(u, n):
        return piece(u + n // 2, lax.rem(n, 2))

    def projections(side):
        @pl.loop(0, 2)
        def _(n):
            p = 4 * side + 2 * n
            k = dot(cn[...], piece(3 * side + KEY, n)).astype(BF)
            keys[p] = k[:, :128]
            keys[p + 1] = k[:, 128:]
            v = dot(cn[...], piece(3 * side + VALUE, n)).astype(BF)
            vals[p, :, 0:128] = v[:, :128]
            vals[p + 1, :, 0:128] = v[:, 128:]

            @pl.loop(0, 2)
            def _(m):
                rows = pl.ds(pl.multiple_of(m * (M // 2), M // 2), M // 2)
                q = dot(ln[rows], piece(3 * side + QUERY, n)).astype(BF) * 0.125
                queries[p, rows] = q[:, :128]
                queries[p + 1, rows] = q[:, 128:]

    projections(0)
    gather.fourth(3, 4, 5)
    gather.second(*early)
    gather.first(*late)
    gather.ready(3, 4, 5)
    projections(1)
    T = 128
    low_t = lanes(T) < 64

    @pl.loop(0, H // 2)
    def _(p):
        for r in range(M // T):
            rows = slice(r * T, r * T + T)
            q = queries[p, rows]
            outs = []
            st = stat[rows]
            for t in range(2):
                qt = jnp.where(low_t if t == 0 else ~low_t, q, jnp.zeros_like(q))
                s = dot_t(qt, keys[p]) + bias[rows]
                top = jnp.max(s, axis=1, keepdims=True)
                e = jnp.exp(s - top).astype(BF)
                o = dot(e, vals[p])
                total = o[:, 128:256]
                outs.append(o[:, 0:128] / total)
                st = jnp.where(lanes(T) == 2 * p + t, top + jnp.log(total), st)
            both = jnp.where(low_t, outs[0], outs[1]).astype(BF)
            part[p, r // 2, 2 * (r % 2)] = both[:R]
            part[p, r // 2, 2 * (r % 2) + 1] = both[R:]
            stat[rows] = st

        for a in range(2):
            @pl.when(lax.rem(p, 2) == a)
            def _():
                for i in range(1, K):
                    to = gather.along(a, i)
                    src = part.at[p, to[0]] if a == 0 else part.at[p, :, to[1]]
                    pltpu.make_async_remote_copy(
                        src_ref=src, dst_ref=got1.at[a, i - 1, p // 2],
                        send_sem=rs_send.at[0], recv_sem=rs_recv.at[0, a, i - 1],
                        device_id=gather.device(to), device_id_type=MESH,
                    ).start()

        @pl.when(p == 2)
        def _():
            gather.third(8, 9)

        @pl.when(p == 4)
        def _():
            gather.third(6, 7)

        @pl.when(p == 6)
        def _():
            gather.second(*late)

    for s in range(N):
        fold[s // K, s % K] = folded(stat[s * R : s * R + R])

    def hop(k, a, i, src, dst):
        return pltpu.make_async_remote_copy(
            src_ref=src, dst_ref=dst, send_sem=rs_send.at[k], recv_sem=rs_recv.at[k, a, i - 1],
            device_id=gather.device(gather.along(a, i)), device_id_type=MESH,
        )

    for a in range(2):
        for i in range(1, K):
            to = gather.along(a, i)
            src = fold.at[to[0]] if a == 0 else fold.at[:, to[1]]
            hop(1, a, i, src, gf1.at[a, i - 1]).start()
    gather.fourth(8, 9)

    def spread(a, q):
        lane = lax.broadcasted_iota(jnp.int32, (128, 128), 1)
        row = lax.broadcasted_iota(jnp.int32, (128, 128), 0)
        return (row == 4 * q + 2 * a + lane // 64).astype(F32).astype(BF)

    def weights_of(levels):
        top = functools.reduce(jnp.maximum, levels)
        ws = [jnp.exp(x - top).astype(BF).astype(F32) for x in levels]
        return ws, top + jnp.log(functools.reduce(jnp.add, ws))

    def blend(ws, parts, a, q):
        spreader = spread(a, q)
        total = None
        for wt, o in zip(ws, parts):
            wide = dot(wt, spreader)
            term = wide * o.astype(F32)
            total = (term, wide) if total is None else (total[0] + term, total[1] + wide)
        return total[0] / total[1]

    for a in range(2):
        for i in range(1, K):
            hop(0, a, i, got1.at[a, i - 1], got1.at[a, i - 1]).wait_recv()
            hop(1, a, i, gf1.at[a, i - 1], gf1.at[a, i - 1]).wait_recv()

        @pl.loop(0, K)
        def _(b):
            mine = fold[here[0], b] if a == 0 else fold[b, here[1]]
            ws, level = weights_of([mine] + [gf1[a, i, b] for i in range(3)])
            mf[a, b] = level
            ws = [unfolded(x).astype(BF) for x in ws]
            for q in range(4):
                own = part[2 * q + a, here[0], b] if a == 0 else part[2 * q + a, b, here[1]]
                mid[a, q, b] = blend(ws, [own] + [got1[a, i, q, b] for i in range(3)], a, q).astype(BF)

        for i in range(1, K):
            to = gather.along(1 - a, i)
            b = to[1 - a]
            hop(2, 1 - a, i, mid.at[a, :, b], got2.at[a, i - 1]).start()
            hop(3, 1 - a, i, mf.at[a, b], gf2.at[a, i - 1]).start()

    gather.fourth(6, 7)
    own_rows = pl.ds(pl.multiple_of(me * R, R), R)
    hid[...] = lat[own_rows]
    for a in range(2):
        for i in range(1, K):
            hop(2, 1 - a, i, got2.at[a, i - 1], got2.at[a, i - 1]).wait_recv()
            hop(3, 1 - a, i, gf2.at[a, i - 1], gf2.at[a, i - 1]).wait_recv()
        b = here[1 - a]
        ws, _ = weights_of([mf[a, b]] + [gf2[a, i] for i in range(3)])
        ws = [unfolded(x).astype(BF) for x in ws]
        for q in range(4):
            p = 2 * q + a
            att[:, 128 * p : 128 * p + 128] = blend(
                ws, [mid[a, q, b]] + [got2[a, i, q] for i in range(3)], a, q
            ).astype(BF)
    gather.ready(*early)

    def add_update(rows_ref, u):
        @pl.loop(0, D // 256)
        def _(n):
            cols = pl.ds(pl.multiple_of(n * 256, 256), 256)
            update = dot(rows_ref[...], unit(u, n))
            hid[:, cols] = (hid[:, cols].astype(F32) + update).astype(BF)

    add_update(att, OUT)
    low = lanes(R) < 64
    half = R // 2
    lo = lanes(half) < 64
    rest = pl.ds(0, N - 1)

    def give(l, t, to, src, dst):
        @pl.when(to != me)
        def _():
            pltpu.make_async_remote_copy(
                src_ref=src.at[to], dst_ref=dst.at[l, me],
                send_sem=lsend_sem.at[l, t], recv_sem=lrecv_sem.at[l, t],
                device_id={"seq": to}, device_id_type=MESH,
            ).start()

    def taken(l, t, dst):
        return push(me, 1, dst.at[l, rest], dst.at[l, rest], lsend_sem.at[l, t], lrecv_sem.at[l, t])

    for l in range(2):
        units = LAYER_UNITS[l]
        if l == 1:
            taken(0, 0, qk_in).wait_send()
            taken(0, 1, v_in).wait_send()
            taken(0, 2, m_in).wait_send()
        norm[...] = normed_rows(hid[...], lg[l : l + 1])

        @pl.loop(0, 4)
        def _(step):
            n = lax.rem(step + me // 4 + 1, 4)
            q4 = dot(norm[...], unit(units[0], n)).astype(BF) * 0.125
            k4 = dot(norm[...], unit(units[1], n)).astype(BF)
            v4 = dot(norm[...], unit(units[2], n)).astype(BF)
            for j in range(2):
                q, k, v = (a[:, 128 * j : 128 * j + 128] for a in (q4, k4, v4))
                to = 4 * n + 2 * j
                qk_out[to] = jnp.where(low, q, roll(k))
                qk_out[to + 1] = jnp.where(low, roll(q), k)
                vr = roll(v)
                v_out[to] = jnp.where(lo, v[:half], vr[half:])
                v_out[to + 1] = jnp.where(lo, vr[:half], v[half:])
            for j in range(4):
                give(l, 0, 4 * n + j, qk_out, qk_in)
                give(l, 1, 4 * n + j, v_out, v_in)

        qk_in[l, me] = qk_out[me]
        v_in[l, me] = v_out[me]
        if l == 0:
            gather.third(*late)
        taken(l, 0, qk_in).wait_recv()
        taken(l, 1, v_in).wait_recv()

        qk = qk_in[l].reshape(M, 128)
        kk = roll(qk)
        vp = v_in[l]
        vr = roll(vp.reshape(M // 2, 128)).reshape(N, half, 128)
        both = jnp.concatenate([vp, vr], axis=1).reshape(M, 128)
        vv = jnp.where(lanes(M) < 64, both, jnp.ones_like(both))
        for r in reversed(range(M // T)):
            size = (r + 1) * T
            q = qk[r * T : size]
            q = jnp.where(low_t, q, jnp.zeros_like(q))
            s = dot_t(q, kk[:size])
            i = lax.broadcasted_iota(jnp.int32, (T, size), 0) + r * T
            j = lax.broadcasted_iota(jnp.int32, (T, size), 1)
            s = jnp.where(j <= i, s, NEGATIVE)
            top = jnp.max(s, axis=1, keepdims=True)
            e = jnp.exp(s - top).astype(BF)
            o = dot(e, vv[:size])
            mixed = o / pltpu.roll(o, 64, 1)
            other = pltpu.roll(mixed, 64, 1)
            for t in range(T // R):
                to = r * (T // R) + t
                m_out[to] = jnp.where(
                    lo, mixed[t * R : t * R + half], other[t * R + half : t * R + R]
                ).astype(BF)
        for step in range(1, N):
            push(
                me, step, m_out.at[lax.rem(me + step, N)], m_in.at[l, me],
                lsend_sem.at[l, 2], lrecv_sem.at[l, 2],
            ).start()
        m_in[l, me] = m_out[me]
        if l == 0:
            gather.fourth(*late)
        taken(l, 2, m_in).wait_recv()
        for p in range(H // 2):
            a = m_in[l, 2 * p]
            b = m_in[l, 2 * p + 1]
            merged[0:half, 128 * p : 128 * p + 128] = jnp.where(lo, a, roll(b))
            merged[half:R, 128 * p : 128 * p + 128] = jnp.where(lo, roll(a), b)
        if l == 0:
            gather.ready(*late)
        add_update(merged, units[3])

    out_ref[0] = hid[...]
    hop(0, 0, 1, got1, got1).wait_send()
    hop(1, 0, 1, gf1, gf1).wait_send()
    hop(2, 0, 1, got2, got2).wait_send()
    hop(3, 0, 1, gf2, gf2).wait_send()
    taken(1, 0, qk_in).wait_send()
    taken(1, 1, v_in).wait_send()
    taken(1, 2, m_in).wait_send()
    gather.close()


VM = pl.BlockSpec(memory_space=pltpu.VMEM)
SM = pl.BlockSpec(memory_space=pltpu.SMEM)
ANY = pl.BlockSpec(memory_space=pl.ANY)
DMA = pltpu.SemaphoreType.DMA


def per_device(
    context,
    latents,
    offsets,
    query_gain,
    key_gain,
    layer_gain,
    cross_query,
    cross_key,
    cross_value,
    cross_out,
    layer_qkv,
    layer_out,
):
    C, M = context.shape[1], latents.shape[1]
    R = M // N
    G = len(GROUPS)
    most = max(g[1] for g in GROUPS)
    return pl.pallas_call(
        kernel,
        out_shape=jax.ShapeDtypeStruct((1, R, D), BF),
        in_specs=[SM] + [ANY] * 11,
        out_specs=VM,
        scratch_shapes=[
            pltpu.VMEM((C, D), BF),
            pltpu.VMEM((M, D), BF),
            pltpu.VMEM((1, D), F32),
            pltpu.VMEM((1, D), F32),
            pltpu.VMEM((2, D), F32),
            pltpu.VMEM((24, K, K, K, 2, 8, HALF), BF),
            pltpu.VMEM(((K * K - 1) * most, 8, HALF), BF),
            pltpu.VMEM((C, D), BF),
            pltpu.VMEM((M, D), BF),
            pltpu.VMEM((H // 2, C, 128), BF),
            pltpu.VMEM((H // 2, C, 256), BF),
            pltpu.VMEM((H // 2, M, 128), BF),
            pltpu.VMEM((M, C), F32),
            pltpu.VMEM((H // 2, K, K, R, 128), BF),
            pltpu.VMEM((M, 128), F32),
            pltpu.VMEM((K, K, 8, 128), F32),
            pltpu.VMEM((2, K - 1, 4, K, R, 128), BF),
            pltpu.VMEM((2, K - 1, K, 8, 128), F32),
            pltpu.VMEM((2, 4, K, R, 128), BF),
            pltpu.VMEM((2, K, 8, 128), F32),
            pltpu.VMEM((2, K - 1, 4, R, 128), BF),
            pltpu.VMEM((2, K - 1, 8, 128), F32),
            pltpu.VMEM((R, D), BF),
            pltpu.VMEM((R, D), BF),
            pltpu.VMEM((R, D), BF),
            pltpu.VMEM((H, R, 128), BF),
            pltpu.VMEM((H, R // 2, 128), BF),
            pltpu.VMEM((2, N, R, 128), BF),
            pltpu.VMEM((2, N, R // 2, 128), BF),
            pltpu.VMEM((N, R // 2, 128), BF),
            pltpu.VMEM((2, H, R // 2, 128), BF),
            pltpu.VMEM((R, D), BF),
            DMA((5,)),
            DMA((24,)),
            DMA((G,)),
            DMA((G,)),
            DMA((G, 2)),
            DMA((G, 2)),
            DMA((G,)),
            DMA((G, 5)),
            DMA((4,)),
            DMA((4, 2, 3)),
            DMA((2, 3)),
            DMA((2, 3)),
        ],
        compiler_params=pltpu.CompilerParams(
            collective_id=0, has_side_effects=True, vmem_limit_bytes=60 << 20
        ),
        name="window",
    )(
        offsets, context, latents, query_gain[None], key_gain[None], layer_gain,
        cross_query, cross_key, cross_value, cross_out, layer_qkv, layer_out,
    )

def solution(mesh):
    return jax.shard_map(
        per_device,
        mesh=mesh,
        in_specs=(
            P("head", "seq", None),
            P("head", None, None),
            P("head"),
            P(),
            P(),
            P(),
            P(("seq", "head"), None),
            P(("seq", "head"), None),
            P(("seq", "head"), None),
            P(("seq", "head"), None),
            P(None, ("seq", "head"), None),
            P(None, ("seq", "head"), None),
        ),
        out_specs=P("head", "seq", None),
        check_vma=False,
    )
```

```python
import functools

import jax
import jax.numpy as jnp
from jax import lax
from jax.experimental import pallas as pl
from jax.experimental.pallas import tpu as pltpu
from jax.sharding import PartitionSpec as P

H = 16
EPSILON = 1e-06
NEGATIVE = -1e30
BF = jnp.bfloat16
F32 = jnp.float32
MESH = pl.DeviceIdType.MESH
N = 16
D = 1024


def normed_rows(x, gain):
    x = x.astype(F32)
    scale = lax.rsqrt(jnp.mean(x * x, axis=-1, keepdims=True) + EPSILON)
    return (x * scale * gain).astype(BF)


def dot(a, b):
    return jnp.dot(a, b, preferred_element_type=F32)


def dot_t(a, b):
    return lax.dot_general(a, b, (((1,), (1,)), ((), ())), preferred_element_type=F32)


def lanes(rows, width=128):
    return lax.broadcasted_iota(jnp.int32, (rows, width), 1)


K = 4
X, Z, Y = 0, 1, 2
GROUPS = (
    (0, 1, X, Y, Z, 0),
    (1, 1, Y, X, Z, 0),
    (2, 1, Z, X, Y, 0),
    (3, 1, X, Y, Z, 0),
    (4, 1, Y, X, Z, 0),
    (5, 1, Z, X, Y, 0),
    (6, 2, Y, X, Z, 1),
    (8, 2, Y, Z, X, 1),
    (10, 2, X, Y, Z, 1),
    (12, 2, Z, Y, X, 1),
    (14, 2, Y, X, Z, 1),
    (16, 2, Y, Z, X, 1),
    (18, 2, X, Y, Z, 1),
    (20, 2, Z, Y, X, 1),
    (22, 2, Y, X, Z, 1),
)


class Gather:
    def __init__(self, w, blank, sems):
        self.w, self.blank = w, blank
        self.line_sem, self.near_sem, self.side_sem, self.far_sem, self.mate_sem, self.sent_sem = sems
        me, lane = lax.axis_index("seq"), lax.axis_index("head")
        self.me = me
        self.at = (me // K, lax.rem(me, K), lane // 2)
        self.core = lax.rem(lane, 2)

    def device(self, at, core=None):
        core = self.core if core is None else core
        return {"seq": at[0] * K + at[1], "head": at[2] * 2 + core}

    def mate(self):
        return self.device(self.at, 1 - self.core)

    def plane(self, axis):
        a, b = [i for i in range(3) if i != axis]
        flat = self.at[a] * K + self.at[b]

        def peer(i):
            j = lax.rem(flat + i, K * K)
            at = list(self.at)
            at[a], at[b] = j // K, lax.rem(j, K)
            return at

        return peer

    def along(self, axis, step):
        at = list(self.at)
        at[axis] = lax.rem(at[axis] + step, K)
        return at

    def units(self, g):
        return pl.ds(GROUPS[g][0], GROUPS[g][1])

    def own(self, g):
        return self.w.at[(self.units(g), *self.at, self.core)]

    def line(self, g):
        index = list(self.at)
        index[GROUPS[g][3]] = slice(None)
        return self.w.at[(self.units(g), *index, self.core)]

    def slab(self, g, step, half=None):
        axis = GROUPS[g][2]
        index = [slice(None)] * 3
        index[axis] = lax.rem(self.at[axis] + step, K)
        if half is not None:
            index[1 if axis == 0 else 0] = pl.ds(2 * half, 2)
        return self.w.at[(self.units(g), *index, self.core)]

    def copy(self, ref, sent, recv, device):
        return pltpu.make_async_remote_copy(
            src_ref=ref, dst_ref=ref, send_sem=sent, recv_sem=recv,
            device_id=device, device_id_type=MESH,
        )

    def wait_for(self, ref, sem):
        self.copy(ref, self.sent_sem.at[0, 0], sem, self.mate()).wait_recv()

    def blanks(self, g, n):
        return self.blank.at[pl.ds(0, n * GROUPS[g][1])]

    def to_mate(self, g, step):
        self.copy(
            self.slab(g, step), self.sent_sem.at[g, 3], self.mate_sem.at[g], self.mate()
        ).start()

    def greet(self):
        barrier = pltpu.get_barrier_semaphore()
        for axis in range(3):
            peer = self.plane(axis)

            @pl.loop(1, K * K)
            def _(i):
                pl.semaphore_signal(
                    barrier, inc=1, device_id=self.device(peer(i)), device_id_type=MESH
                )

        pl.semaphore_signal(barrier, inc=1, device_id=self.mate(), device_id_type=MESH)
        pl.semaphore_wait(barrier, 3 * (K * K - 1) + 1)

    def begin(self, *groups):
        for g in groups:
            _, k, axis, first, second, steps = GROUPS[g]
            if steps:
                for i in range(1, K):
                    self.copy(
                        self.own(g), self.sent_sem.at[g, 4], self.line_sem.at[g],
                        self.device(self.along(first, i)),
                    ).start()
            else:
                peer = self.plane(axis)

                @pl.loop(1, K * K)
                def _(i):
                    self.copy(
                        self.own(g), self.sent_sem.at[g, 0], self.near_sem.at[g],
                        self.device(peer(i)),
                    ).start()

    def first(self, *groups):
        for g in groups:
            self.wait_for(self.blanks(g, K - 1), self.line_sem.at[g])
            for i in range(1, K):
                self.copy(
                    self.line(g), self.sent_sem.at[g, 0], self.near_sem.at[g],
                    self.device(self.along(GROUPS[g][4], i)),
                ).start()

    def second(self, *groups):
        for g in groups:
            n = K * (K - 1) if GROUPS[g][5] else K * K - 1
            self.wait_for(self.blanks(g, n), self.near_sem.at[g])
            for side, step in enumerate((1, 3)):
                self.copy(
                    self.slab(g, 0), self.sent_sem.at[g, 1],
                    self.side_sem.at[g, side], self.device(self.along(GROUPS[g][2], step)),
                ).start()
        for g in groups:
            self.to_mate(g, 0)

    def third(self, *groups):
        for g in groups:
            for side, step in enumerate((1, 3)):
                self.wait_for(self.slab(g, 4 - step), self.side_sem.at[g, side])
                self.copy(
                    self.slab(g, 4 - step, side), self.sent_sem.at[g, 2],
                    self.far_sem.at[g, side], self.device(self.along(GROUPS[g][2], step)),
                ).start()
        for g in groups:
            self.to_mate(g, 1)
            self.to_mate(g, 3)

    def fourth(self, *groups):
        for g in groups:
            for side in range(2):
                self.wait_for(self.slab(g, 2, side), self.far_sem.at[g, side])
            self.to_mate(g, 2)

    def ready(self, *groups):
        for g in groups:
            self.wait_for(
                self.w.at[(self.units(g), slice(None), slice(None), slice(None), self.core)],
                self.mate_sem.at[g],
            )

    def close(self):
        full = slice(None)
        for g in range(len(GROUPS)):
            units = self.units(g)
            steps = GROUPS[g][5]
            ends = [
                (0, self.blanks(g, K * (K - 1) if steps else K * K - 1)),
                (1, self.w.at[(units, pl.ds(0, 2), full, full, self.core)]),
                (2, self.w.at[(units, pl.ds(0, 1), full, full, self.core)]),
                (3, self.w.at[(units, full, full, full, self.core)]),
            ]
            if steps:
                ends.append((4, self.blanks(g, K - 1)))
            for phase, ref in ends:
                self.copy(ref, self.sent_sem.at[g, phase], self.near_sem.at[g], self.mate()).wait_send()


def push(me, d, src, dst, send_sem, recv_sem):
    return pltpu.make_async_remote_copy(
        src_ref=src,
        dst_ref=dst,
        send_sem=send_sem,
        recv_sem=recv_sem,
        device_id={"seq": lax.rem(me + d, N)},
        device_id_type=MESH,
    )


def roll(a):
    return pltpu.roll(a.astype(F32), 64, 1).astype(BF)


def folded(block):
    out = block[0:8]
    for t in range(1, 8):
        out = out + pltpu.roll(block[8 * t : 8 * t + 8], 16 * t, 1)
    return out


def unfolded(small):
    return jnp.concatenate(
        [small] + [pltpu.roll(small, 128 - 16 * t, 1) for t in range(1, 8)], axis=0
    )


KEY, VALUE, QUERY = 0, 1, 2
OUT = 6
LAYER_UNITS = ((8, 10, 12, 14), (16, 18, 20, 22))
HALF = D // 2


def kernel(
    off_ref, ctx_any, lat_any, qg_any, kg_any, lg_any, cq_any, ck_any, cv_any, co_any, lq_any, lo_any,
    out_ref,
    ctx, lat, qg, kg, lg, w, blank, cn, ln, keys, vals, queries, bias, part, stat, fold,
    got1, gf1, mid, mf, got2, gf2,
    att, hid, norm, qk_out, v_out, qk_in, v_in, m_out, m_in, merged,
    load_sem, shard_sem, line_sem, near_sem, side_sem, far_sem, mate_sem, sent_sem,
    rs_send, rs_recv, lsend_sem, lrecv_sem,
):
    me = lax.axis_index("seq")
    gather = Gather(w, blank, (line_sem, near_sem, side_sem, far_sem, mate_sem, sent_sem))
    here = gather.at
    shards = [a.at[:, pl.ds(HALF * t, HALF)] for t in range(2) for a in (ck_any, cv_any, cq_any)]
    shards += [co_any.at[:, pl.ds(HALF * t, HALF)] for t in range(2)]
    for l in range(2):
        shards += [lq_any.at[l, :, pl.ds(HALF * t, HALF)] for t in range(6)]
        shards += [lo_any.at[l, :, pl.ds(HALF * t, HALF)] for t in range(2)]
    shards = [
        pltpu.make_async_copy(s, w.at[(u, *here, gather.core)], shard_sem.at[u])
        for u, s in enumerate(shards)
    ]
    loads = [
        pltpu.make_async_copy(a, b, load_sem.at[i])
        for i, (a, b) in enumerate((
            (kg_any, kg), (ctx_any.at[0], ctx), (qg_any, qg), (lat_any.at[0], lat), (lg_any, lg),
        ))
    ]
    for c in shards[:6] + loads + shards[6:]:
        c.start()
    gather.greet()
    for c in shards[:6]:
        c.wait()
    gather.begin(0, 1, 2)
    gather.begin(3, 4, 5)
    early, late = (6, 7, 8, 9), (10, 11, 12, 13, 14)
    for c in shards[6:]:
        c.wait()
    gather.begin(*early)
    C = ctx.shape[0]
    M = lat.shape[0]
    R = M // N
    S = 128
    edge = me * C - off_ref[0]
    loads[0].wait()
    loads[1].wait()

    @pl.loop(0, C // S)
    def _(r):
        rows = pl.ds(pl.multiple_of(r * S, S), S)
        cn[rows] = normed_rows(ctx[rows], kg[...])

    stat[...] = jnp.zeros_like(stat)
    vals[:, :, 128:256] = jnp.ones((H // 2, C, 128), BF)
    for c in loads[2:]:
        c.wait()
    gather.second(0, 1, 2)

    @pl.loop(0, M // S)
    def _(r):
        rows = pl.ds(pl.multiple_of(r * S, S), S)
        ln[rows] = normed_rows(lat[rows], qg[...])
        i = lax.broadcasted_iota(jnp.int32, (S, C), 0) + r * S
        j = lax.broadcasted_iota(jnp.int32, (S, C), 1)
        bias[rows] = jnp.where(j + edge <= i, 0.0, NEGATIVE)

    gather.second(3, 4, 5)
    gather.third(0, 1, 2)
    gather.third(3, 4, 5)
    gather.begin(*late)
    gather.fourth(0, 1, 2)
    gather.first(*early)
    gather.ready(0, 1, 2)

    def piece(u, n):
        cols = pl.ds(pl.multiple_of(n * 256, 256), 256)
        return w[u, :, :, :, :, :, cols].reshape(D, 256)

    def unit(u, n):
        return piece(u + n // 2, lax.rem(n, 2))

    def projections(side):
        @pl.loop(0, 2)
        def _(n):
            p = 4 * side + 2 * n
            k = dot(cn[...], piece(3 * side + KEY, n)).astype(BF)
            keys[p] = k[:, :128]
            keys[p + 1] = k[:, 128:]
            v = dot(cn[...], piece(3 * side + VALUE, n)).astype(BF)
            vals[p, :, 0:128] = v[:, :128]
            vals[p + 1, :, 0:128] = v[:, 128:]

            @pl.loop(0, 2)
            def _(m):
                rows = pl.ds(pl.multiple_of(m * (M // 2), M // 2), M // 2)
                q = dot(ln[rows], piece(3 * side + QUERY, n)).astype(BF) * 0.125
                queries[p, rows] = q[:, :128]
                queries[p + 1, rows] = q[:, 128:]

    projections(0)
    gather.fourth(3, 4, 5)
    gather.second(6, 7)
    gather.first(10, 11)
    gather.ready(3, 4, 5)
    projections(1)
    gather.second(8, 9)
    gather.first(12, 13, 14)
    T = 128
    low_t = lanes(T) < 64

    @pl.loop(0, H // 2)
    def _(p):
        for r in range(M // T):
            rows = slice(r * T, r * T + T)
            q = queries[p, rows]
            outs = []
            st = stat[rows]
            for t in range(2):
                qt = jnp.where(low_t if t == 0 else ~low_t, q, jnp.zeros_like(q))
                s = dot_t(qt, keys[p]) + bias[rows]
                top = jnp.max(s, axis=1, keepdims=True)
                e = jnp.exp(s - top).astype(BF)
                o = dot(e, vals[p])
                total = o[:, 128:256]
                outs.append(o[:, 0:128] / total)
                st = jnp.where(lanes(T) == 2 * p + t, top + jnp.log(total), st)
            both = jnp.where(low_t, outs[0], outs[1]).astype(BF)
            part[p, r // 2, 2 * (r % 2)] = both[:R]
            part[p, r // 2, 2 * (r % 2) + 1] = both[R:]
            stat[rows] = st

        for a in range(2):
            @pl.when(lax.rem(p, 2) == a)
            def _():
                for i in range(1, K):
                    to = gather.along(a, i)
                    src = part.at[p, to[0]] if a == 0 else part.at[p, :, to[1]]
                    pltpu.make_async_remote_copy(
                        src_ref=src, dst_ref=got1.at[a, i - 1, p // 2],
                        send_sem=rs_send.at[0], recv_sem=rs_recv.at[0, a, i - 1],
                        device_id=gather.device(to), device_id_type=MESH,
                    ).start()

        @pl.when(p == 1)
        def _():
            gather.third(6)

        @pl.when(p == 2)
        def _():
            gather.second(10, 11)

        @pl.when(p == 3)
        def _():
            gather.third(7)

        @pl.when(p == 5)
        def _():
            gather.third(8, 9)

    for s in range(N):
        fold[s // K, s % K] = folded(stat[s * R : s * R + R])

    def hop(k, a, i, src, dst):
        return pltpu.make_async_remote_copy(
            src_ref=src, dst_ref=dst, send_sem=rs_send.at[k], recv_sem=rs_recv.at[k, a, i - 1],
            device_id=gather.device(gather.along(a, i)), device_id_type=MESH,
        )

    for a in range(2):
        for i in range(1, K):
            to = gather.along(a, i)
            src = fold.at[to[0]] if a == 0 else fold.at[:, to[1]]
            hop(1, a, i, src, gf1.at[a, i - 1]).start()

    def spread(a, q):
        lane = lax.broadcasted_iota(jnp.int32, (128, 128), 1)
        row = lax.broadcasted_iota(jnp.int32, (128, 128), 0)
        return (row == 4 * q + 2 * a + lane // 64).astype(F32).astype(BF)

    def weights_of(levels):
        top = functools.reduce(jnp.maximum, levels)
        ws = [jnp.exp(x - top).astype(BF).astype(F32) for x in levels]
        return ws, top + jnp.log(functools.reduce(jnp.add, ws))

    def blend(ws, parts, a, q):
        spreader = spread(a, q)
        total = None
        for wt, o in zip(ws, parts):
            wide = dot(wt, spreader)
            term = wide * o.astype(F32)
            total = (term, wide) if total is None else (total[0] + term, total[1] + wide)
        return total[0] / total[1]

    for a in range(2):
        for i in range(1, K):
            hop(0, a, i, got1.at[a, i - 1], got1.at[a, i - 1]).wait_recv()
            hop(1, a, i, gf1.at[a, i - 1], gf1.at[a, i - 1]).wait_recv()

        @pl.loop(0, K)
        def _(b):
            mine = fold[here[0], b] if a == 0 else fold[b, here[1]]
            ws, level = weights_of([mine] + [gf1[a, i, b] for i in range(3)])
            mf[a, b] = level
            ws = [unfolded(x).astype(BF) for x in ws]
            for q in range(4):
                own = part[2 * q + a, here[0], b] if a == 0 else part[2 * q + a, b, here[1]]
                mid[a, q, b] = blend(ws, [own] + [got1[a, i, q, b] for i in range(3)], a, q).astype(BF)

        for i in range(1, K):
            to = gather.along(1 - a, i)
            b = to[1 - a]
            hop(2, 1 - a, i, mid.at[a, :, b], got2.at[a, i - 1]).start()
            hop(3, 1 - a, i, mf.at[a, b], gf2.at[a, i - 1]).start()

    gather.fourth(*early)
    gather.second(12, 13, 14)
    gather.third(10, 11)
    own_rows = pl.ds(pl.multiple_of(me * R, R), R)
    hid[...] = lat[own_rows]
    for a in range(2):
        for i in range(1, K):
            hop(2, 1 - a, i, got2.at[a, i - 1], got2.at[a, i - 1]).wait_recv()
            hop(3, 1 - a, i, gf2.at[a, i - 1], gf2.at[a, i - 1]).wait_recv()
        b = here[1 - a]
        ws, _ = weights_of([mf[a, b]] + [gf2[a, i] for i in range(3)])
        ws = [unfolded(x).astype(BF) for x in ws]
        for q in range(4):
            p = 2 * q + a
            att[:, 128 * p : 128 * p + 128] = blend(
                ws, [mid[a, q, b]] + [got2[a, i, q] for i in range(3)], a, q
            ).astype(BF)
    gather.ready(*early)

    def add_update(rows_ref, u):
        @pl.loop(0, D // 256)
        def _(n):
            cols = pl.ds(pl.multiple_of(n * 256, 256), 256)
            update = dot(rows_ref[...], unit(u, n))
            hid[:, cols] = (hid[:, cols].astype(F32) + update).astype(BF)

    add_update(att, OUT)
    low = lanes(R) < 64
    half = R // 2
    lo = lanes(half) < 64
    rest = pl.ds(0, N - 1)

    def give(l, t, to, src, dst):
        @pl.when(to != me)
        def _():
            pltpu.make_async_remote_copy(
                src_ref=src.at[to], dst_ref=dst.at[l, me],
                send_sem=lsend_sem.at[l, t], recv_sem=lrecv_sem.at[l, t],
                device_id={"seq": to}, device_id_type=MESH,
            ).start()

    def taken(l, t, dst):
        return push(me, 1, dst.at[l, rest], dst.at[l, rest], lsend_sem.at[l, t], lrecv_sem.at[l, t])

    for l in range(2):
        units = LAYER_UNITS[l]
        if l == 1:
            gather.ready(11, 12, 13)
            taken(0, 0, qk_in).wait_send()
            taken(0, 1, v_in).wait_send()
            taken(0, 2, m_in).wait_send()
        norm[...] = normed_rows(hid[...], lg[l : l + 1])

        @pl.loop(0, 4)
        def _(step):
            n = lax.rem(step + me // 4 + 1, 4)
            q4 = dot(norm[...], unit(units[0], n)).astype(BF) * 0.125
            k4 = dot(norm[...], unit(units[1], n)).astype(BF)
            v4 = dot(norm[...], unit(units[2], n)).astype(BF)
            for j in range(2):
                q, k, v = (a[:, 128 * j : 128 * j + 128] for a in (q4, k4, v4))
                to = 4 * n + 2 * j
                qk_out[to] = jnp.where(low, q, roll(k))
                qk_out[to + 1] = jnp.where(low, roll(q), k)
                vr = roll(v)
                v_out[to] = jnp.where(lo, v[:half], vr[half:])
                v_out[to + 1] = jnp.where(lo, vr[:half], v[half:])
            for j in range(4):
                give(l, 0, 4 * n + j, qk_out, qk_in)
                give(l, 1, 4 * n + j, v_out, v_in)

        qk_in[l, me] = qk_out[me]
        v_in[l, me] = v_out[me]
        if l == 0:
            gather.third(12, 13)
            gather.fourth(10, 11)
        else:
            gather.fourth(14)
        taken(l, 0, qk_in).wait_recv()
        taken(l, 1, v_in).wait_recv()

        qk = qk_in[l].reshape(M, 128)
        kk = roll(qk)
        vp = v_in[l]
        vr = roll(vp.reshape(M // 2, 128)).reshape(N, half, 128)
        both = jnp.concatenate([vp, vr], axis=1).reshape(M, 128)
        vv = jnp.where(lanes(M) < 64, both, jnp.ones_like(both))
        for r in reversed(range(M // T)):
            size = (r + 1) * T
            q = qk[r * T : size]
            q = jnp.where(low_t, q, jnp.zeros_like(q))
            s = dot_t(q, kk[:size])
            i = lax.broadcasted_iota(jnp.int32, (T, size), 0) + r * T
            j = lax.broadcasted_iota(jnp.int32, (T, size), 1)
            s = jnp.where(j <= i, s, NEGATIVE)
            top = jnp.max(s, axis=1, keepdims=True)
            e = jnp.exp(s - top).astype(BF)
            o = dot(e, vv[:size])
            mixed = o / pltpu.roll(o, 64, 1)
            other = pltpu.roll(mixed, 64, 1)
            for t in range(T // R):
                to = r * (T // R) + t
                m_out[to] = jnp.where(
                    lo, mixed[t * R : t * R + half], other[t * R + half : t * R + R]
                ).astype(BF)
        for step in range(1, N):
            push(
                me, step, m_out.at[lax.rem(me + step, N)], m_in.at[l, me],
                lsend_sem.at[l, 2], lrecv_sem.at[l, 2],
            ).start()
        m_in[l, me] = m_out[me]
        if l == 0:
            gather.third(14)
            gather.fourth(12, 13)
        taken(l, 2, m_in).wait_recv()
        for p in range(H // 2):
            a = m_in[l, 2 * p]
            b = m_in[l, 2 * p + 1]
            merged[0:half, 128 * p : 128 * p + 128] = jnp.where(lo, a, roll(b))
            merged[half:R, 128 * p : 128 * p + 128] = jnp.where(lo, roll(a), b)
        gather.ready(10 if l == 0 else 14)
        add_update(merged, units[3])

    out_ref[0] = hid[...]
    hop(0, 0, 1, got1, got1).wait_send()
    hop(1, 0, 1, gf1, gf1).wait_send()
    hop(2, 0, 1, got2, got2).wait_send()
    hop(3, 0, 1, gf2, gf2).wait_send()
    taken(1, 0, qk_in).wait_send()
    taken(1, 1, v_in).wait_send()
    taken(1, 2, m_in).wait_send()
    gather.close()


VM = pl.BlockSpec(memory_space=pltpu.VMEM)
SM = pl.BlockSpec(memory_space=pltpu.SMEM)
ANY = pl.BlockSpec(memory_space=pl.ANY)
DMA = pltpu.SemaphoreType.DMA


def per_device(
    context,
    latents,
    offsets,
    query_gain,
    key_gain,
    layer_gain,
    cross_query,
    cross_key,
    cross_value,
    cross_out,
    layer_qkv,
    layer_out,
):
    C, M = context.shape[1], latents.shape[1]
    R = M // N
    G = len(GROUPS)
    most = max(g[1] for g in GROUPS)
    return pl.pallas_call(
        kernel,
        out_shape=jax.ShapeDtypeStruct((1, R, D), BF),
        in_specs=[SM] + [ANY] * 11,
        out_specs=VM,
        scratch_shapes=[
            pltpu.VMEM((C, D), BF),
            pltpu.VMEM((M, D), BF),
            pltpu.VMEM((1, D), F32),
            pltpu.VMEM((1, D), F32),
            pltpu.VMEM((2, D), F32),
            pltpu.VMEM((24, K, K, K, 2, 8, HALF), BF),
            pltpu.VMEM(((K * K - 1) * most, 8, HALF), BF),
            pltpu.VMEM((C, D), BF),
            pltpu.VMEM((M, D), BF),
            pltpu.VMEM((H // 2, C, 128), BF),
            pltpu.VMEM((H // 2, C, 256), BF),
            pltpu.VMEM((H // 2, M, 128), BF),
            pltpu.VMEM((M, C), F32),
            pltpu.VMEM((H // 2, K, K, R, 128), BF),
            pltpu.VMEM((M, 128), F32),
            pltpu.VMEM((K, K, 8, 128), F32),
            pltpu.VMEM((2, K - 1, 4, K, R, 128), BF),
            pltpu.VMEM((2, K - 1, K, 8, 128), F32),
            pltpu.VMEM((2, 4, K, R, 128), BF),
            pltpu.VMEM((2, K, 8, 128), F32),
            pltpu.VMEM((2, K - 1, 4, R, 128), BF),
            pltpu.VMEM((2, K - 1, 8, 128), F32),
            pltpu.VMEM((R, D), BF),
            pltpu.VMEM((R, D), BF),
            pltpu.VMEM((R, D), BF),
            pltpu.VMEM((H, R, 128), BF),
            pltpu.VMEM((H, R // 2, 128), BF),
            pltpu.VMEM((2, N, R, 128), BF),
            pltpu.VMEM((2, N, R // 2, 128), BF),
            pltpu.VMEM((N, R // 2, 128), BF),
            pltpu.VMEM((2, H, R // 2, 128), BF),
            pltpu.VMEM((R, D), BF),
            DMA((5,)),
            DMA((24,)),
            DMA((G,)),
            DMA((G,)),
            DMA((G, 2)),
            DMA((G, 2)),
            DMA((G,)),
            DMA((G, 5)),
            DMA((4,)),
            DMA((4, 2, 3)),
            DMA((2, 3)),
            DMA((2, 3)),
        ],
        compiler_params=pltpu.CompilerParams(
            collective_id=0, has_side_effects=True, vmem_limit_bytes=60 << 20
        ),
        name="window",
    )(
        offsets, context, latents, query_gain[None], key_gain[None], layer_gain,
        cross_query, cross_key, cross_value, cross_out, layer_qkv, layer_out,
    )

def solution(mesh):
    return jax.shard_map(
        per_device,
        mesh=mesh,
        in_specs=(
            P("head", "seq", None),
            P("head", None, None),
            P("head"),
            P(),
            P(),
            P(),
            P(("seq", "head"), None),
            P(("seq", "head"), None),
            P(("seq", "head"), None),
            P(("seq", "head"), None),
            P(None, ("seq", "head"), None),
            P(None, ("seq", "head"), None),
        ),
        out_specs=P("head", "seq", None),
        check_vma=False,
    )
```

```python
import functools

import jax
import jax.numpy as jnp
from jax import lax
from jax.experimental import pallas as pl
from jax.experimental.pallas import tpu as pltpu
from jax.sharding import PartitionSpec as P

H = 16
EPSILON = 1e-06
NEGATIVE = -1e30
BF = jnp.bfloat16
F32 = jnp.float32
MESH = pl.DeviceIdType.MESH
N = 16
D = 1024


def normed_rows(x, gain):
    x = x.astype(F32)
    scale = lax.rsqrt(jnp.mean(x * x, axis=-1, keepdims=True) + EPSILON)
    return (x * scale * gain).astype(BF)


def dot(a, b):
    return jnp.dot(a, b, preferred_element_type=F32)


def dot_t(a, b):
    return lax.dot_general(a, b, (((1,), (1,)), ((), ())), preferred_element_type=F32)


def lanes(rows, width=128):
    return lax.broadcasted_iota(jnp.int32, (rows, width), 1)


K = 4
X, Z, Y = 0, 1, 2
GROUPS = (
    (0, 1, X, Y, Z, 0),
    (1, 1, Y, X, Z, 0),
    (2, 1, Z, X, Y, 0),
    (3, 1, X, Y, Z, 0),
    (4, 1, Y, X, Z, 0),
    (5, 1, Z, X, Y, 0),
    (6, 2, Y, X, Z, 1),
    (8, 2, Y, Z, X, 1),
    (10, 2, X, Y, Z, 1),
    (12, 2, Z, Y, X, 1),
    (14, 2, Y, X, Z, 1),
    (16, 2, Y, Z, X, 1),
    (18, 2, X, Y, Z, 1),
    (20, 2, Z, Y, X, 1),
    (22, 2, Y, X, Z, 1),
)


class Gather:
    def __init__(self, w, blank, sems):
        self.w, self.blank = w, blank
        self.line_sem, self.near_sem, self.side_sem, self.far_sem, self.mate_sem, self.sent_sem = sems
        me, lane = lax.axis_index("seq"), lax.axis_index("head")
        self.me = me
        self.at = (me // K, lax.rem(me, K), lane // 2)
        self.core = lax.rem(lane, 2)

    def device(self, at, core=None):
        core = self.core if core is None else core
        return {"seq": at[0] * K + at[1], "head": at[2] * 2 + core}

    def mate(self):
        return self.device(self.at, 1 - self.core)

    def plane(self, axis):
        a, b = [i for i in range(3) if i != axis]
        flat = self.at[a] * K + self.at[b]

        def peer(i):
            j = lax.rem(flat + i, K * K)
            at = list(self.at)
            at[a], at[b] = j // K, lax.rem(j, K)
            return at

        return peer

    def along(self, axis, step):
        at = list(self.at)
        at[axis] = lax.rem(at[axis] + step, K)
        return at

    def units(self, g):
        return pl.ds(GROUPS[g][0], GROUPS[g][1])

    def own(self, g):
        return self.w.at[(self.units(g), *self.at, self.core)]

    def line(self, g):
        index = list(self.at)
        index[GROUPS[g][3]] = slice(None)
        return self.w.at[(self.units(g), *index, self.core)]

    def slab(self, g, step, half=None):
        axis = GROUPS[g][2]
        index = [slice(None)] * 3
        index[axis] = lax.rem(self.at[axis] + step, K)
        if half is not None:
            index[1 if axis == 0 else 0] = pl.ds(2 * half, 2)
        return self.w.at[(self.units(g), *index, self.core)]

    def copy(self, ref, sent, recv, device):
        return pltpu.make_async_remote_copy(
            src_ref=ref, dst_ref=ref, send_sem=sent, recv_sem=recv,
            device_id=device, device_id_type=MESH,
        )

    def wait_for(self, ref, sem):
        self.copy(ref, self.sent_sem.at[0, 0], sem, self.mate()).wait_recv()

    def blanks(self, g, n):
        return self.blank.at[pl.ds(0, n * GROUPS[g][1])]

    def to_mate(self, g, step):
        self.copy(
            self.slab(g, step), self.sent_sem.at[g, 3], self.mate_sem.at[g], self.mate()
        ).start()

    def greet(self):
        barrier = pltpu.get_barrier_semaphore()
        for axis in range(3):
            peer = self.plane(axis)

            @pl.loop(1, K * K)
            def _(i):
                pl.semaphore_signal(
                    barrier, inc=1, device_id=self.device(peer(i)), device_id_type=MESH
                )

        pl.semaphore_signal(barrier, inc=1, device_id=self.mate(), device_id_type=MESH)
        pl.semaphore_wait(barrier, 3 * (K * K - 1) + 1)

    def begin(self, *groups):
        for g in groups:
            _, k, axis, first, second, steps = GROUPS[g]
            if steps:
                for i in range(1, K):
                    self.copy(
                        self.own(g), self.sent_sem.at[g, 4], self.line_sem.at[g],
                        self.device(self.along(first, i)),
                    ).start()
            else:
                peer = self.plane(axis)

                @pl.loop(1, K * K)
                def _(i):
                    self.copy(
                        self.own(g), self.sent_sem.at[g, 0], self.near_sem.at[g],
                        self.device(peer(i)),
                    ).start()

    def first(self, *groups):
        for g in groups:
            self.wait_for(self.blanks(g, K - 1), self.line_sem.at[g])
            for i in range(1, K):
                self.copy(
                    self.line(g), self.sent_sem.at[g, 0], self.near_sem.at[g],
                    self.device(self.along(GROUPS[g][4], i)),
                ).start()

    def second(self, *groups):
        for g in groups:
            n = K * (K - 1) if GROUPS[g][5] else K * K - 1
            self.wait_for(self.blanks(g, n), self.near_sem.at[g])
            for side, step in enumerate((1, 3)):
                self.copy(
                    self.slab(g, 0), self.sent_sem.at[g, 1],
                    self.side_sem.at[g, side], self.device(self.along(GROUPS[g][2], step)),
                ).start()
        for g in groups:
            self.to_mate(g, 0)

    def third(self, *groups):
        for g in groups:
            for side, step in enumerate((1, 3)):
                self.wait_for(self.slab(g, 4 - step), self.side_sem.at[g, side])
                self.copy(
                    self.slab(g, 4 - step, side), self.sent_sem.at[g, 2],
                    self.far_sem.at[g, side], self.device(self.along(GROUPS[g][2], step)),
                ).start()
        for g in groups:
            self.to_mate(g, 1)
            self.to_mate(g, 3)

    def fourth(self, *groups):
        for g in groups:
            for side in range(2):
                self.wait_for(self.slab(g, 2, side), self.far_sem.at[g, side])
            self.to_mate(g, 2)

    def ready(self, *groups):
        for g in groups:
            self.wait_for(
                self.w.at[(self.units(g), slice(None), slice(None), slice(None), self.core)],
                self.mate_sem.at[g],
            )

    def close(self):
        full = slice(None)
        for g in range(len(GROUPS)):
            units = self.units(g)
            steps = GROUPS[g][5]
            ends = [
                (0, self.blanks(g, K * (K - 1) if steps else K * K - 1)),
                (1, self.w.at[(units, pl.ds(0, 2), full, full, self.core)]),
                (2, self.w.at[(units, pl.ds(0, 1), full, full, self.core)]),
                (3, self.w.at[(units, full, full, full, self.core)]),
            ]
            if steps:
                ends.append((4, self.blanks(g, K - 1)))
            for phase, ref in ends:
                self.copy(ref, self.sent_sem.at[g, phase], self.near_sem.at[g], self.mate()).wait_send()


def push(me, d, src, dst, send_sem, recv_sem):
    return pltpu.make_async_remote_copy(
        src_ref=src,
        dst_ref=dst,
        send_sem=send_sem,
        recv_sem=recv_sem,
        device_id={"seq": lax.rem(me + d, N)},
        device_id_type=MESH,
    )


def roll(a):
    return pltpu.roll(a.astype(F32), 64, 1).astype(BF)


def folded(block):
    out = block[0:8]
    for t in range(1, 8):
        out = out + pltpu.roll(block[8 * t : 8 * t + 8], 16 * t, 1)
    return out


def unfolded(small):
    return jnp.concatenate(
        [small] + [pltpu.roll(small, 128 - 16 * t, 1) for t in range(1, 8)], axis=0
    )


KEY, VALUE, QUERY = 0, 1, 2
OUT = 6
LAYER_UNITS = ((8, 10, 12, 14), (16, 18, 20, 22))
HALF = D // 2


def kernel(
    off_ref, ctx_any, lat_any, qg_any, kg_any, lg_any, cq_any, ck_any, cv_any, co_any, lq_any, lo_any,
    out_ref,
    ctx, lat, qg, kg, lg, w, blank, cn, ln, keys, vals, queries, bias, part, stat, fold,
    got1, gf1, mid, mf, got2, gf2,
    att, hid, norm, qk_out, v_out, qk_in, v_in, m_out, m_in, merged,
    load_sem, shard_sem, line_sem, near_sem, side_sem, far_sem, mate_sem, sent_sem,
    rs_send, rs_recv, lsend_sem, lrecv_sem,
):
    me = lax.axis_index("seq")
    gather = Gather(w, blank, (line_sem, near_sem, side_sem, far_sem, mate_sem, sent_sem))
    here = gather.at
    shards = [a.at[:, pl.ds(HALF * t, HALF)] for t in range(2) for a in (ck_any, cv_any, cq_any)]
    shards += [co_any.at[:, pl.ds(HALF * t, HALF)] for t in range(2)]
    for l in range(2):
        shards += [lq_any.at[l, :, pl.ds(HALF * t, HALF)] for t in range(6)]
        shards += [lo_any.at[l, :, pl.ds(HALF * t, HALF)] for t in range(2)]
    shards = [
        pltpu.make_async_copy(s, w.at[(u, *here, gather.core)], shard_sem.at[u])
        for u, s in enumerate(shards)
    ]
    loads = [
        pltpu.make_async_copy(a, b, load_sem.at[i])
        for i, (a, b) in enumerate((
            (kg_any, kg), (ctx_any.at[0], ctx), (qg_any, qg), (lat_any.at[0], lat), (lg_any, lg),
        ))
    ]
    for c in shards[:6] + loads + shards[6:]:
        c.start()
    gather.greet()
    for c in shards[:6]:
        c.wait()
    gather.begin(0, 1, 2)
    gather.begin(3, 4, 5)
    early, late = (6, 7, 8, 9), (10, 11, 12, 13, 14)
    for c in shards[6:]:
        c.wait()
    gather.begin(*early)
    C = ctx.shape[0]
    M = lat.shape[0]
    R = M // N
    S = 128
    edge = me * C - off_ref[0]
    loads[0].wait()
    loads[1].wait()

    @pl.loop(0, C // S)
    def _(r):
        rows = pl.ds(pl.multiple_of(r * S, S), S)
        cn[rows] = normed_rows(ctx[rows], kg[...])

    stat[...] = jnp.zeros_like(stat)
    vals[:, :, 128:256] = jnp.ones((H // 2, C, 128), BF)
    for c in loads[2:]:
        c.wait()
    gather.second(0, 1, 2)

    @pl.loop(0, M // S)
    def _(r):
        rows = pl.ds(pl.multiple_of(r * S, S), S)
        ln[rows] = normed_rows(lat[rows], qg[...])
        i = lax.broadcasted_iota(jnp.int32, (S, C), 0) + r * S
        j = lax.broadcasted_iota(jnp.int32, (S, C), 1)
        bias[rows] = jnp.where(j + edge <= i, 0.0, NEGATIVE)

    gather.second(3, 4, 5)
    gather.third(0, 1, 2)
    gather.third(3, 4, 5)
    gather.begin(*late)
    gather.fourth(0, 1, 2)
    gather.first(*early)
    gather.ready(0, 1, 2)

    def piece(u, n):
        cols = pl.ds(pl.multiple_of(n * 256, 256), 256)
        return w[u, :, :, :, :, :, cols].reshape(D, 256)

    def unit(u, n):
        return piece(u + n // 2, lax.rem(n, 2))

    def projections(side):
        @pl.loop(0, 2)
        def _(n):
            p = 4 * side + 2 * n
            k = dot(cn[...], piece(3 * side + KEY, n)).astype(BF)
            keys[p] = k[:, :128]
            keys[p + 1] = k[:, 128:]
            v = dot(cn[...], piece(3 * side + VALUE, n)).astype(BF)
            vals[p, :, 0:128] = v[:, :128]
            vals[p + 1, :, 0:128] = v[:, 128:]

            @pl.loop(0, 2, unroll=2)
            def _(m):
                rows = pl.ds(pl.multiple_of(m * (M // 2), M // 2), M // 2)
                q = dot(ln[rows], piece(3 * side + QUERY, n)).astype(BF) * 0.125
                queries[p, rows] = q[:, :128]
                queries[p + 1, rows] = q[:, 128:]

    projections(0)
    gather.fourth(3, 4, 5)
    gather.second(6, 7)
    gather.first(10, 11)
    gather.ready(3, 4, 5)
    projections(1)
    gather.second(8, 9)
    gather.first(12, 13, 14)
    T = 128
    low_t = lanes(T) < 64

    @pl.loop(0, H // 2)
    def _(p):
        for r in range(M // T):
            rows = slice(r * T, r * T + T)
            q = queries[p, rows]
            outs = []
            st = stat[rows]
            for t in range(2):
                qt = jnp.where(low_t if t == 0 else ~low_t, q, jnp.zeros_like(q))
                s = dot_t(qt, keys[p]) + bias[rows]
                top = jnp.max(s, axis=1, keepdims=True)
                e = jnp.exp(s - top).astype(BF)
                o = dot(e, vals[p])
                total = o[:, 128:256]
                outs.append(o[:, 0:128] / total)
                st = jnp.where(lanes(T) == 2 * p + t, top + jnp.log(total), st)
            both = jnp.where(low_t, outs[0], outs[1]).astype(BF)
            part[p, r // 2, 2 * (r % 2)] = both[:R]
            part[p, r // 2, 2 * (r % 2) + 1] = both[R:]
            stat[rows] = st

        for a in range(2):
            @pl.when(lax.rem(p, 2) == a)
            def _():
                for i in range(1, K):
                    to = gather.along(a, i)
                    src = part.at[p, to[0]] if a == 0 else part.at[p, :, to[1]]
                    pltpu.make_async_remote_copy(
                        src_ref=src, dst_ref=got1.at[a, i - 1, p // 2],
                        send_sem=rs_send.at[0], recv_sem=rs_recv.at[0, a, i - 1],
                        device_id=gather.device(to), device_id_type=MESH,
                    ).start()

        @pl.when(p == 1)
        def _():
            gather.third(6)

        @pl.when(p == 2)
        def _():
            gather.second(10, 11)

        @pl.when(p == 3)
        def _():
            gather.third(7)

        @pl.when(p == 5)
        def _():
            gather.third(8, 9)

    for s in range(N):
        fold[s // K, s % K] = folded(stat[s * R : s * R + R])

    def hop(k, a, i, src, dst):
        return pltpu.make_async_remote_copy(
            src_ref=src, dst_ref=dst, send_sem=rs_send.at[k], recv_sem=rs_recv.at[k, a, i - 1],
            device_id=gather.device(gather.along(a, i)), device_id_type=MESH,
        )

    for a in range(2):
        for i in range(1, K):
            to = gather.along(a, i)
            src = fold.at[to[0]] if a == 0 else fold.at[:, to[1]]
            hop(1, a, i, src, gf1.at[a, i - 1]).start()

    def spread(a, q):
        lane = lax.broadcasted_iota(jnp.int32, (128, 128), 1)
        row = lax.broadcasted_iota(jnp.int32, (128, 128), 0)
        return (row == 4 * q + 2 * a + lane // 64).astype(F32).astype(BF)

    def weights_of(levels):
        top = functools.reduce(jnp.maximum, levels)
        ws = [jnp.exp(x - top).astype(BF).astype(F32) for x in levels]
        return ws, top + jnp.log(functools.reduce(jnp.add, ws))

    def blend(ws, parts, a, q):
        spreader = spread(a, q)
        total = None
        for wt, o in zip(ws, parts):
            wide = dot(wt, spreader)
            term = wide * o.astype(F32)
            total = (term, wide) if total is None else (total[0] + term, total[1] + wide)
        return total[0] / total[1]

    for a in range(2):
        for i in range(1, K):
            hop(0, a, i, got1.at[a, i - 1], got1.at[a, i - 1]).wait_recv()
            hop(1, a, i, gf1.at[a, i - 1], gf1.at[a, i - 1]).wait_recv()

        @pl.loop(0, K, unroll=K)
        def _(b):
            mine = fold[here[0], b] if a == 0 else fold[b, here[1]]
            ws, level = weights_of([mine] + [gf1[a, i, b] for i in range(3)])
            mf[a, b] = level
            ws = [unfolded(x).astype(BF) for x in ws]
            for q in range(4):
                own = part[2 * q + a, here[0], b] if a == 0 else part[2 * q + a, b, here[1]]
                mid[a, q, b] = blend(ws, [own] + [got1[a, i, q, b] for i in range(3)], a, q).astype(BF)

        for i in range(1, K):
            to = gather.along(1 - a, i)
            b = to[1 - a]
            hop(2, 1 - a, i, mid.at[a, :, b], got2.at[a, i - 1]).start()
            hop(3, 1 - a, i, mf.at[a, b], gf2.at[a, i - 1]).start()

    gather.fourth(*early)
    gather.second(12, 13, 14)
    gather.third(10, 11)
    own_rows = pl.ds(pl.multiple_of(me * R, R), R)
    hid[...] = lat[own_rows]
    for a in range(2):
        for i in range(1, K):
            hop(2, 1 - a, i, got2.at[a, i - 1], got2.at[a, i - 1]).wait_recv()
            hop(3, 1 - a, i, gf2.at[a, i - 1], gf2.at[a, i - 1]).wait_recv()
        b = here[1 - a]
        ws, _ = weights_of([mf[a, b]] + [gf2[a, i] for i in range(3)])
        ws = [unfolded(x).astype(BF) for x in ws]
        for q in range(4):
            p = 2 * q + a
            att[:, 128 * p : 128 * p + 128] = blend(
                ws, [mid[a, q, b]] + [got2[a, i, q] for i in range(3)], a, q
            ).astype(BF)
    gather.ready(6)

    def add_update(rows_ref, u):
        @pl.loop(0, D // 256, unroll=D // 256)
        def _(n):
            cols = pl.ds(pl.multiple_of(n * 256, 256), 256)
            update = dot(rows_ref[...], unit(u, n))
            hid[:, cols] = (hid[:, cols].astype(F32) + update).astype(BF)

    add_update(att, OUT)
    gather.ready(7, 8, 9)
    low = lanes(R) < 64
    half = R // 2
    lo = lanes(half) < 64
    rest = pl.ds(0, N - 1)

    def give(l, t, to, src, dst):
        @pl.when(to != me)
        def _():
            pltpu.make_async_remote_copy(
                src_ref=src.at[to], dst_ref=dst.at[l, me],
                send_sem=lsend_sem.at[l, t], recv_sem=lrecv_sem.at[l, t],
                device_id={"seq": to}, device_id_type=MESH,
            ).start()

    def taken(l, t, dst):
        return push(me, 1, dst.at[l, rest], dst.at[l, rest], lsend_sem.at[l, t], lrecv_sem.at[l, t])

    for l in range(2):
        units = LAYER_UNITS[l]
        if l == 1:
            gather.ready(11, 12, 13)
            taken(0, 0, qk_in).wait_send()
            taken(0, 1, v_in).wait_send()
            taken(0, 2, m_in).wait_send()
        norm[...] = normed_rows(hid[...], lg[l : l + 1])

        @pl.loop(0, 4)
        def _(step):
            n = lax.rem(step + me // 4 + 1, 4)
            q4 = dot(norm[...], unit(units[0], n)).astype(BF) * 0.125
            k4 = dot(norm[...], unit(units[1], n)).astype(BF)
            v4 = dot(norm[...], unit(units[2], n)).astype(BF)
            for j in range(2):
                q, k, v = (a[:, 128 * j : 128 * j + 128] for a in (q4, k4, v4))
                to = 4 * n + 2 * j
                qk_out[to] = jnp.where(low, q, roll(k))
                qk_out[to + 1] = jnp.where(low, roll(q), k)
                vr = roll(v)
                v_out[to] = jnp.where(lo, v[:half], vr[half:])
                v_out[to + 1] = jnp.where(lo, vr[:half], v[half:])
            for j in range(4):
                give(l, 0, 4 * n + j, qk_out, qk_in)
                give(l, 1, 4 * n + j, v_out, v_in)

        qk_in[l, me] = qk_out[me]
        v_in[l, me] = v_out[me]
        if l == 0:
            gather.third(12, 13)
            gather.fourth(10, 11)
        else:
            gather.fourth(14)
        taken(l, 0, qk_in).wait_recv()
        taken(l, 1, v_in).wait_recv()

        qk = qk_in[l].reshape(M, 128)
        kk = roll(qk)
        vp = v_in[l]
        vr = roll(vp.reshape(M // 2, 128)).reshape(N, half, 128)
        both = jnp.concatenate([vp, vr], axis=1).reshape(M, 128)
        vv = jnp.where(lanes(M) < 64, both, jnp.ones_like(both))
        for r in reversed(range(M // T)):
            size = (r + 1) * T
            q = qk[r * T : size]
            q = jnp.where(low_t, q, jnp.zeros_like(q))
            s = dot_t(q, kk[:size])
            i = lax.broadcasted_iota(jnp.int32, (T, size), 0) + r * T
            j = lax.broadcasted_iota(jnp.int32, (T, size), 1)
            s = jnp.where(j <= i, s, NEGATIVE)
            top = jnp.max(s, axis=1, keepdims=True)
            e = jnp.exp(s - top).astype(BF)
            o = dot(e, vv[:size])
            mixed = o / pltpu.roll(o, 64, 1)
            other = pltpu.roll(mixed, 64, 1)
            for t in range(T // R):
                to = r * (T // R) + t
                m_out[to] = jnp.where(
                    lo, mixed[t * R : t * R + half], other[t * R + half : t * R + R]
                ).astype(BF)
        for step in range(1, N):
            push(
                me, step, m_out.at[lax.rem(me + step, N)], m_in.at[l, me],
                lsend_sem.at[l, 2], lrecv_sem.at[l, 2],
            ).start()
        m_in[l, me] = m_out[me]
        if l == 0:
            gather.third(14)
            gather.fourth(12, 13)
        taken(l, 2, m_in).wait_recv()
        for p in range(H // 2):
            a = m_in[l, 2 * p]
            b = m_in[l, 2 * p + 1]
            merged[0:half, 128 * p : 128 * p + 128] = jnp.where(lo, a, roll(b))
            merged[half:R, 128 * p : 128 * p + 128] = jnp.where(lo, roll(a), b)
        gather.ready(10 if l == 0 else 14)
        add_update(merged, units[3])

    out_ref[0] = hid[...]
    hop(0, 0, 1, got1, got1).wait_send()
    hop(1, 0, 1, gf1, gf1).wait_send()
    hop(2, 0, 1, got2, got2).wait_send()
    hop(3, 0, 1, gf2, gf2).wait_send()
    taken(1, 0, qk_in).wait_send()
    taken(1, 1, v_in).wait_send()
    taken(1, 2, m_in).wait_send()
    gather.close()


VM = pl.BlockSpec(memory_space=pltpu.VMEM)
SM = pl.BlockSpec(memory_space=pltpu.SMEM)
ANY = pl.BlockSpec(memory_space=pl.ANY)
DMA = pltpu.SemaphoreType.DMA


def per_device(
    context,
    latents,
    offsets,
    query_gain,
    key_gain,
    layer_gain,
    cross_query,
    cross_key,
    cross_value,
    cross_out,
    layer_qkv,
    layer_out,
):
    C, M = context.shape[1], latents.shape[1]
    R = M // N
    G = len(GROUPS)
    most = max(g[1] for g in GROUPS)
    return pl.pallas_call(
        kernel,
        out_shape=jax.ShapeDtypeStruct((1, R, D), BF),
        in_specs=[SM] + [ANY] * 11,
        out_specs=VM,
        scratch_shapes=[
            pltpu.VMEM((C, D), BF),
            pltpu.VMEM((M, D), BF),
            pltpu.VMEM((1, D), F32),
            pltpu.VMEM((1, D), F32),
            pltpu.VMEM((2, D), F32),
            pltpu.VMEM((24, K, K, K, 2, 8, HALF), BF),
            pltpu.VMEM(((K * K - 1) * most, 8, HALF), BF),
            pltpu.VMEM((C, D), BF),
            pltpu.VMEM((M, D), BF),
            pltpu.VMEM((H // 2, C, 128), BF),
            pltpu.VMEM((H // 2, C, 256), BF),
            pltpu.VMEM((H // 2, M, 128), BF),
            pltpu.VMEM((M, C), F32),
            pltpu.VMEM((H // 2, K, K, R, 128), BF),
            pltpu.VMEM((M, 128), F32),
            pltpu.VMEM((K, K, 8, 128), F32),
            pltpu.VMEM((2, K - 1, 4, K, R, 128), BF),
            pltpu.VMEM((2, K - 1, K, 8, 128), F32),
            pltpu.VMEM((2, 4, K, R, 128), BF),
            pltpu.VMEM((2, K, 8, 128), F32),
            pltpu.VMEM((2, K - 1, 4, R, 128), BF),
            pltpu.VMEM((2, K - 1, 8, 128), F32),
            pltpu.VMEM((R, D), BF),
            pltpu.VMEM((R, D), BF),
            pltpu.VMEM((R, D), BF),
            pltpu.VMEM((H, R, 128), BF),
            pltpu.VMEM((H, R // 2, 128), BF),
            pltpu.VMEM((2, N, R, 128), BF),
            pltpu.VMEM((2, N, R // 2, 128), BF),
            pltpu.VMEM((N, R // 2, 128), BF),
            pltpu.VMEM((2, H, R // 2, 128), BF),
            pltpu.VMEM((R, D), BF),
            DMA((5,)),
            DMA((24,)),
            DMA((G,)),
            DMA((G,)),
            DMA((G, 2)),
            DMA((G, 2)),
            DMA((G,)),
            DMA((G, 5)),
            DMA((4,)),
            DMA((4, 2, 3)),
            DMA((2, 3)),
            DMA((2, 3)),
        ],
        compiler_params=pltpu.CompilerParams(
            collective_id=0, has_side_effects=True, vmem_limit_bytes=60 << 20
        ),
        name="window",
    )(
        offsets, context, latents, query_gain[None], key_gain[None], layer_gain,
        cross_query, cross_key, cross_value, cross_out, layer_qkv, layer_out,
    )

def solution(mesh):
    return jax.shard_map(
        per_device,
        mesh=mesh,
        in_specs=(
            P("head", "seq", None),
            P("head", None, None),
            P("head"),
            P(),
            P(),
            P(),
            P(("seq", "head"), None),
            P(("seq", "head"), None),
            P(("seq", "head"), None),
            P(("seq", "head"), None),
            P(None, ("seq", "head"), None),
            P(None, ("seq", "head"), None),
        ),
        out_specs=P("head", "seq", None),
        check_vma=False,
    )
```

```python
import functools

import jax
import jax.numpy as jnp
from jax import lax
from jax.experimental import pallas as pl
from jax.experimental.pallas import tpu as pltpu
from jax.sharding import PartitionSpec as P

H = 16
EPSILON = 1e-06
NEGATIVE = -1e30
BF = jnp.bfloat16
F32 = jnp.float32
MESH = pl.DeviceIdType.MESH
N = 16
D = 1024


def normed_rows(x, gain):
    x = x.astype(F32)
    scale = lax.rsqrt(jnp.mean(x * x, axis=-1, keepdims=True) + EPSILON)
    return (x * scale * gain).astype(BF)


def dot(a, b):
    return jnp.dot(a, b, preferred_element_type=F32)


def dot_t(a, b):
    return lax.dot_general(a, b, (((1,), (1,)), ((), ())), preferred_element_type=F32)


def lanes(rows, width=128):
    return lax.broadcasted_iota(jnp.int32, (rows, width), 1)


K = 4
X, Z, Y = 0, 1, 2
GROUPS = (
    (0, 1, X, Y, Z, 0),
    (1, 1, Y, X, Z, 0),
    (2, 1, Z, X, Y, 0),
    (3, 1, X, Y, Z, 0),
    (4, 1, Y, X, Z, 0),
    (5, 1, Z, X, Y, 0),
    (6, 2, Y, X, Z, 1),
    (8, 2, Y, Z, X, 1),
    (10, 2, X, Y, Z, 1),
    (12, 2, Z, Y, X, 1),
    (14, 2, Y, X, Z, 1),
    (16, 2, Y, Z, X, 1),
    (18, 2, X, Y, Z, 1),
    (20, 2, Z, Y, X, 1),
    (22, 2, Y, X, Z, 1),
)


class Gather:
    def __init__(self, w, blank, sems):
        self.w, self.blank = w, blank
        self.line_sem, self.near_sem, self.side_sem, self.far_sem, self.mate_sem, self.sent_sem = sems
        me, lane = lax.axis_index("seq"), lax.axis_index("head")
        self.me = me
        self.at = (me // K, lax.rem(me, K), lane // 2)
        self.core = lax.rem(lane, 2)

    def device(self, at, core=None):
        core = self.core if core is None else core
        return {"seq": at[0] * K + at[1], "head": at[2] * 2 + core}

    def mate(self):
        return self.device(self.at, 1 - self.core)

    def plane(self, axis):
        a, b = [i for i in range(3) if i != axis]
        flat = self.at[a] * K + self.at[b]

        def peer(i):
            j = lax.rem(flat + i, K * K)
            at = list(self.at)
            at[a], at[b] = j // K, lax.rem(j, K)
            return at

        return peer

    def along(self, axis, step):
        at = list(self.at)
        at[axis] = lax.rem(at[axis] + step, K)
        return at

    def units(self, g):
        return pl.ds(GROUPS[g][0], GROUPS[g][1])

    def own(self, g):
        return self.w.at[(self.units(g), *self.at, self.core)]

    def line(self, g):
        index = list(self.at)
        index[GROUPS[g][3]] = slice(None)
        return self.w.at[(self.units(g), *index, self.core)]

    def slab(self, g, step, half=None):
        axis = GROUPS[g][2]
        index = [slice(None)] * 3
        index[axis] = lax.rem(self.at[axis] + step, K)
        if half is not None:
            index[1 if axis == 0 else 0] = pl.ds(2 * half, 2)
        return self.w.at[(self.units(g), *index, self.core)]

    def copy(self, ref, sent, recv, device):
        return pltpu.make_async_remote_copy(
            src_ref=ref, dst_ref=ref, send_sem=sent, recv_sem=recv,
            device_id=device, device_id_type=MESH,
        )

    def wait_for(self, ref, sem):
        self.copy(ref, self.sent_sem.at[0, 0], sem, self.mate()).wait_recv()

    def blanks(self, g, n):
        return self.blank.at[pl.ds(0, n * GROUPS[g][1])]

    def to_mate(self, g, step):
        self.copy(
            self.slab(g, step), self.sent_sem.at[g, 3], self.mate_sem.at[g], self.mate()
        ).start()

    def greet(self):
        barrier = pltpu.get_barrier_semaphore()
        for axis in range(3):
            peer = self.plane(axis)

            @pl.loop(1, K * K)
            def _(i):
                pl.semaphore_signal(
                    barrier, inc=1, device_id=self.device(peer(i)), device_id_type=MESH
                )

        pl.semaphore_signal(barrier, inc=1, device_id=self.mate(), device_id_type=MESH)
        pl.semaphore_wait(barrier, 3 * (K * K - 1) + 1)

    def begin(self, *groups):
        for g in groups:
            _, k, axis, first, second, steps = GROUPS[g]
            if steps:
                for i in range(1, K):
                    self.copy(
                        self.own(g), self.sent_sem.at[g, 4], self.line_sem.at[g],
                        self.device(self.along(first, i)),
                    ).start()
            else:
                peer = self.plane(axis)

                @pl.loop(1, K * K)
                def _(i):
                    self.copy(
                        self.own(g), self.sent_sem.at[g, 0], self.near_sem.at[g],
                        self.device(peer(i)),
                    ).start()

    def first(self, *groups):
        for g in groups:
            self.wait_for(self.blanks(g, K - 1), self.line_sem.at[g])
            for i in range(1, K):
                self.copy(
                    self.line(g), self.sent_sem.at[g, 0], self.near_sem.at[g],
                    self.device(self.along(GROUPS[g][4], i)),
                ).start()

    def second(self, *groups):
        for g in groups:
            n = K * (K - 1) if GROUPS[g][5] else K * K - 1
            self.wait_for(self.blanks(g, n), self.near_sem.at[g])
            for side, step in enumerate((1, 3)):
                self.copy(
                    self.slab(g, 0), self.sent_sem.at[g, 1],
                    self.side_sem.at[g, side], self.device(self.along(GROUPS[g][2], step)),
                ).start()
        for g in groups:
            self.to_mate(g, 0)

    def third(self, *groups):
        for g in groups:
            for side, step in enumerate((1, 3)):
                self.wait_for(self.slab(g, 4 - step), self.side_sem.at[g, side])
                self.copy(
                    self.slab(g, 4 - step, side), self.sent_sem.at[g, 2],
                    self.far_sem.at[g, side], self.device(self.along(GROUPS[g][2], step)),
                ).start()
        for g in groups:
            self.to_mate(g, 1)
            self.to_mate(g, 3)

    def fourth(self, *groups):
        for g in groups:
            for side in range(2):
                self.wait_for(self.slab(g, 2, side), self.far_sem.at[g, side])
            self.to_mate(g, 2)

    def ready(self, *groups):
        for g in groups:
            self.wait_for(
                self.w.at[(self.units(g), slice(None), slice(None), slice(None), self.core)],
                self.mate_sem.at[g],
            )

    def close(self):
        full = slice(None)
        for g in range(len(GROUPS)):
            units = self.units(g)
            steps = GROUPS[g][5]
            ends = [
                (0, self.blanks(g, K * (K - 1) if steps else K * K - 1)),
                (1, self.w.at[(units, pl.ds(0, 2), full, full, self.core)]),
                (2, self.w.at[(units, pl.ds(0, 1), full, full, self.core)]),
                (3, self.w.at[(units, full, full, full, self.core)]),
            ]
            if steps:
                ends.append((4, self.blanks(g, K - 1)))
            for phase, ref in ends:
                self.copy(ref, self.sent_sem.at[g, phase], self.near_sem.at[g], self.mate()).wait_send()


def push(me, d, src, dst, send_sem, recv_sem):
    return pltpu.make_async_remote_copy(
        src_ref=src,
        dst_ref=dst,
        send_sem=send_sem,
        recv_sem=recv_sem,
        device_id={"seq": lax.rem(me + d, N)},
        device_id_type=MESH,
    )


def roll(a):
    return pltpu.roll(a.astype(F32), 64, 1).astype(BF)


def folded(block):
    out = block[0:8]
    for t in range(1, 8):
        out = out + pltpu.roll(block[8 * t : 8 * t + 8], 16 * t, 1)
    return out


def unfolded(small):
    return jnp.concatenate(
        [small] + [pltpu.roll(small, 128 - 16 * t, 1) for t in range(1, 8)], axis=0
    )


KEY, VALUE, QUERY = 0, 1, 2
OUT = 6
LAYER_UNITS = ((8, 10, 12, 14), (16, 18, 20, 22))
HALF = D // 2


def kernel(
    off_ref, ctx_any, lat_any, qg_any, kg_any, lg_any, cq_any, ck_any, cv_any, co_any, lq_any, lo_any,
    out_ref,
    ctx, lat, qg, kg, lg, w, blank, cn, ln, keys, vals, queries, bias, part, stat, fold,
    got1, gf1, mid, mf, got2, gf2,
    att, hid, norm, qk_out, v_out, qk_in, v_in, m_out, m_in, merged,
    load_sem, shard_sem, line_sem, near_sem, side_sem, far_sem, mate_sem, sent_sem,
    rs_send, rs_recv, lsend_sem, lrecv_sem,
):
    me = lax.axis_index("seq")
    gather = Gather(w, blank, (line_sem, near_sem, side_sem, far_sem, mate_sem, sent_sem))
    here = gather.at
    shards = [a.at[:, pl.ds(HALF * t, HALF)] for t in range(2) for a in (ck_any, cv_any, cq_any)]
    shards += [co_any.at[:, pl.ds(HALF * t, HALF)] for t in range(2)]
    for l in range(2):
        shards += [lq_any.at[l, :, pl.ds(HALF * t, HALF)] for t in range(6)]
        shards += [lo_any.at[l, :, pl.ds(HALF * t, HALF)] for t in range(2)]
    shards = [
        pltpu.make_async_copy(s, w.at[(u, *here, gather.core)], shard_sem.at[u])
        for u, s in enumerate(shards)
    ]
    loads = [
        pltpu.make_async_copy(a, b, load_sem.at[i])
        for i, (a, b) in enumerate((
            (kg_any, kg), (ctx_any.at[0], ctx), (qg_any, qg), (lat_any.at[0], lat), (lg_any, lg),
        ))
    ]
    for c in shards[:6] + loads + shards[6:]:
        c.start()
    gather.greet()
    for c in shards[:6]:
        c.wait()
    gather.begin(0, 1, 2)
    gather.begin(3, 4, 5)
    early, late = (6, 7, 8, 9), (10, 11, 12, 13, 14)
    for c in shards[6:]:
        c.wait()
    gather.begin(*early)
    C = ctx.shape[0]
    M = lat.shape[0]
    R = M // N
    S = 128
    edge = me * C - off_ref[0]
    loads[0].wait()
    loads[1].wait()

    @pl.loop(0, C // S)
    def _(r):
        rows = pl.ds(pl.multiple_of(r * S, S), S)
        cn[rows] = normed_rows(ctx[rows], kg[...])

    stat[...] = jnp.zeros_like(stat)
    vals[:, :, 128:256] = jnp.ones((H // 2, C, 128), BF)
    for c in loads[2:]:
        c.wait()
    gather.second(0, 1, 2)

    @pl.loop(0, M // S)
    def _(r):
        rows = pl.ds(pl.multiple_of(r * S, S), S)
        ln[rows] = normed_rows(lat[rows], qg[...])
        i = lax.broadcasted_iota(jnp.int32, (S, C), 0) + r * S
        j = lax.broadcasted_iota(jnp.int32, (S, C), 1)
        bias[rows] = jnp.where(j + edge <= i, 0.0, NEGATIVE)

    gather.second(3, 4, 5)
    gather.third(0, 1, 2)
    gather.third(3, 4, 5)
    gather.begin(*late)
    gather.fourth(0, 1, 2)
    gather.first(*early)
    gather.ready(0, 1, 2)

    def piece(u, n):
        cols = pl.ds(pl.multiple_of(n * 256, 256), 256)
        return w[u, :, :, :, :, :, cols].reshape(D, 256)

    def unit(u, n):
        return piece(u + n // 2, lax.rem(n, 2))

    def projections(side):
        @pl.loop(0, 2)
        def _(n):
            p = 4 * side + 2 * n
            k = dot(cn[...], piece(3 * side + KEY, n)).astype(BF)
            keys[p] = k[:, :128]
            keys[p + 1] = k[:, 128:]
            v = dot(cn[...], piece(3 * side + VALUE, n)).astype(BF)
            vals[p, :, 0:128] = v[:, :128]
            vals[p + 1, :, 0:128] = v[:, 128:]

            @pl.loop(0, 2, unroll=2)
            def _(m):
                rows = pl.ds(pl.multiple_of(m * (M // 2), M // 2), M // 2)
                q = dot(ln[rows], piece(3 * side + QUERY, n)).astype(BF) * 0.125
                queries[p, rows] = q[:, :128]
                queries[p + 1, rows] = q[:, 128:]

    projections(0)
    gather.fourth(3, 4, 5)
    gather.second(6, 7)
    gather.first(10, 11)
    gather.ready(3, 4, 5)
    projections(1)
    gather.second(8, 9)
    gather.first(12, 13, 14)
    T = 128
    low_t = lanes(T) < 64

    @pl.loop(0, H // 2)
    def _(p):
        for r in range(M // T):
            rows = slice(r * T, r * T + T)
            q = queries[p, rows]
            outs = []
            st = stat[rows]
            for t in range(2):
                qt = jnp.where(low_t if t == 0 else ~low_t, q, jnp.zeros_like(q))
                s = dot_t(qt, keys[p]) + bias[rows]
                top = jnp.max(s, axis=1, keepdims=True)
                e = jnp.exp(s - top).astype(BF)
                o = dot(e, vals[p])
                total = o[:, 128:256]
                outs.append(o[:, 0:128] / total)
                st = jnp.where(lanes(T) == 2 * p + t, top + jnp.log(total), st)
            both = jnp.where(low_t, outs[0], outs[1]).astype(BF)
            part[p, r // 2, 2 * (r % 2)] = both[:R]
            part[p, r // 2, 2 * (r % 2) + 1] = both[R:]
            stat[rows] = st

        for a in range(2):
            @pl.when(lax.rem(p, 2) == a)
            def _():
                for i in range(1, K):
                    to = gather.along(a, i)
                    src = part.at[p, to[0]] if a == 0 else part.at[p, :, to[1]]
                    pltpu.make_async_remote_copy(
                        src_ref=src, dst_ref=got1.at[a, i - 1, p // 2],
                        send_sem=rs_send.at[0], recv_sem=rs_recv.at[0, a, i - 1],
                        device_id=gather.device(to), device_id_type=MESH,
                    ).start()

        @pl.when(p == 1)
        def _():
            gather.third(6)

        @pl.when(p == 2)
        def _():
            gather.second(10, 11)

        @pl.when(p == 3)
        def _():
            gather.third(7)

        @pl.when(p == 5)
        def _():
            gather.third(8, 9)

    for s in range(N):
        fold[s // K, s % K] = folded(stat[s * R : s * R + R])

    def hop(k, a, i, src, dst):
        return pltpu.make_async_remote_copy(
            src_ref=src, dst_ref=dst, send_sem=rs_send.at[k], recv_sem=rs_recv.at[k, a, i - 1],
            device_id=gather.device(gather.along(a, i)), device_id_type=MESH,
        )

    for a in range(2):
        for i in range(1, K):
            to = gather.along(a, i)
            src = fold.at[to[0]] if a == 0 else fold.at[:, to[1]]
            hop(1, a, i, src, gf1.at[a, i - 1]).start()

    def spread(a, q):
        lane = lax.broadcasted_iota(jnp.int32, (128, 128), 1)
        row = lax.broadcasted_iota(jnp.int32, (128, 128), 0)
        return (row == 4 * q + 2 * a + lane // 64).astype(F32).astype(BF)

    def weights_of(levels):
        top = functools.reduce(jnp.maximum, levels)
        ws = [jnp.exp(x - top).astype(BF).astype(F32) for x in levels]
        return ws, top + jnp.log(functools.reduce(jnp.add, ws))

    def blend(ws, parts, a, q):
        spreader = spread(a, q)
        total = None
        for wt, o in zip(ws, parts):
            wide = dot(wt, spreader)
            term = wide * o.astype(F32)
            total = (term, wide) if total is None else (total[0] + term, total[1] + wide)
        return total[0] / total[1]

    for a in range(2):
        for i in range(1, K):
            hop(0, a, i, got1.at[a, i - 1], got1.at[a, i - 1]).wait_recv()
            hop(1, a, i, gf1.at[a, i - 1], gf1.at[a, i - 1]).wait_recv()

        @pl.loop(0, K, unroll=K)
        def _(b):
            mine = fold[here[0], b] if a == 0 else fold[b, here[1]]
            ws, level = weights_of([mine] + [gf1[a, i, b] for i in range(3)])
            mf[a, b] = level
            ws = [unfolded(x).astype(BF) for x in ws]
            for q in range(4):
                own = part[2 * q + a, here[0], b] if a == 0 else part[2 * q + a, b, here[1]]
                mid[a, q, b] = blend(ws, [own] + [got1[a, i, q, b] for i in range(3)], a, q).astype(BF)

        for i in range(1, K):
            to = gather.along(1 - a, i)
            b = to[1 - a]
            hop(2, 1 - a, i, mid.at[a, :, b], got2.at[a, i - 1]).start()
            hop(3, 1 - a, i, mf.at[a, b], gf2.at[a, i - 1]).start()

    gather.fourth(*early)
    gather.second(12, 13, 14)
    gather.third(10, 11)
    own_rows = pl.ds(pl.multiple_of(me * R, R), R)
    hid[...] = lat[own_rows]
    for a in range(2):
        for i in range(1, K):
            hop(2, 1 - a, i, got2.at[a, i - 1], got2.at[a, i - 1]).wait_recv()
            hop(3, 1 - a, i, gf2.at[a, i - 1], gf2.at[a, i - 1]).wait_recv()
        b = here[1 - a]
        ws, _ = weights_of([mf[a, b]] + [gf2[a, i] for i in range(3)])
        ws = [unfolded(x).astype(BF) for x in ws]
        for q in range(4):
            p = 2 * q + a
            att[:, 128 * p : 128 * p + 128] = blend(
                ws, [mid[a, q, b]] + [got2[a, i, q] for i in range(3)], a, q
            ).astype(BF)
    gather.ready(6)

    def add_update(rows_ref, u):
        @pl.loop(0, D // 256, unroll=D // 256)
        def _(n):
            cols = pl.ds(pl.multiple_of(n * 256, 256), 256)
            update = dot(rows_ref[...], unit(u, n))
            hid[:, cols] = (hid[:, cols].astype(F32) + update).astype(BF)

    add_update(att, OUT)
    gather.ready(7, 8, 9)
    low = lanes(R) < 64
    half = R // 2
    lo = lanes(half) < 64
    rest = pl.ds(0, N - 1)

    def give(l, t, to, src, dst, mine):
        def start():
            pltpu.make_async_remote_copy(
                src_ref=src.at[to], dst_ref=dst.at[l, me],
                send_sem=lsend_sem.at[l, t], recv_sem=lrecv_sem.at[l, t],
                device_id={"seq": to}, device_id_type=MESH,
            ).start()

        if mine:
            pl.when(to != me)(start)
        else:
            start()

    def taken(l, t, dst):
        return push(me, 1, dst.at[l, rest], dst.at[l, rest], lsend_sem.at[l, t], lrecv_sem.at[l, t])

    for l in range(2):
        units = LAYER_UNITS[l]
        if l == 1:
            gather.ready(11, 12, 13)
            taken(0, 0, qk_in).wait_send()
            taken(0, 1, v_in).wait_send()
            taken(0, 2, m_in).wait_send()
        norm[...] = normed_rows(hid[...], lg[l : l + 1])

        for step in range(4):
            n = lax.rem(step + me // 4 + 1, 4)
            q4 = dot(norm[...], unit(units[0], n)).astype(BF) * 0.125
            k4 = dot(norm[...], unit(units[1], n)).astype(BF)
            v4 = dot(norm[...], unit(units[2], n)).astype(BF)
            for j in range(2):
                q, k, v = (a[:, 128 * j : 128 * j + 128] for a in (q4, k4, v4))
                to = 4 * n + 2 * j
                qk_out[to] = jnp.where(low, q, roll(k))
                qk_out[to + 1] = jnp.where(low, roll(q), k)
                vr = roll(v)
                v_out[to] = jnp.where(lo, v[:half], vr[half:])
                v_out[to + 1] = jnp.where(lo, vr[:half], v[half:])
            for j in range(4):
                give(l, 0, 4 * n + j, qk_out, qk_in, step == 3)
                give(l, 1, 4 * n + j, v_out, v_in, step == 3)

        qk_in[l, me] = qk_out[me]
        v_in[l, me] = v_out[me]
        if l == 0:
            gather.third(12, 13)
            gather.fourth(10, 11)
        else:
            gather.fourth(14)
        taken(l, 0, qk_in).wait_recv()
        taken(l, 1, v_in).wait_recv()

        qk = qk_in[l].reshape(M, 128)
        kk = roll(qk)
        vp = v_in[l]
        vr = roll(vp.reshape(M // 2, 128)).reshape(N, half, 128)
        both = jnp.concatenate([vp, vr], axis=1).reshape(M, 128)
        vv = jnp.where(lanes(M) < 64, both, jnp.ones_like(both))
        for r in reversed(range(M // T)):
            size = (r + 1) * T
            q = qk[r * T : size]
            q = jnp.where(low_t, q, jnp.zeros_like(q))
            s = dot_t(q, kk[:size])
            i = lax.broadcasted_iota(jnp.int32, (T, size), 0) + r * T
            j = lax.broadcasted_iota(jnp.int32, (T, size), 1)
            s = jnp.where(j <= i, s, NEGATIVE)
            top = jnp.max(s, axis=1, keepdims=True)
            e = jnp.exp(s - top).astype(BF)
            o = dot(e, vv[:size])
            mixed = o / pltpu.roll(o, 64, 1)
            other = pltpu.roll(mixed, 64, 1)
            for t in range(T // R):
                to = r * (T // R) + t
                m_out[to] = jnp.where(
                    lo, mixed[t * R : t * R + half], other[t * R + half : t * R + R]
                ).astype(BF)
        for step in range(1, N):
            push(
                me, step, m_out.at[lax.rem(me + step, N)], m_in.at[l, me],
                lsend_sem.at[l, 2], lrecv_sem.at[l, 2],
            ).start()
        m_in[l, me] = m_out[me]
        if l == 0:
            gather.third(14)
            gather.fourth(12, 13)
        taken(l, 2, m_in).wait_recv()
        for p in range(H // 2):
            a = m_in[l, 2 * p]
            b = m_in[l, 2 * p + 1]
            merged[0:half, 128 * p : 128 * p + 128] = jnp.where(lo, a, roll(b))
            merged[half:R, 128 * p : 128 * p + 128] = jnp.where(lo, roll(a), b)
        gather.ready(10 if l == 0 else 14)
        add_update(merged, units[3])

    out_ref[0] = hid[...]
    hop(0, 0, 1, got1, got1).wait_send()
    hop(1, 0, 1, gf1, gf1).wait_send()
    hop(2, 0, 1, got2, got2).wait_send()
    hop(3, 0, 1, gf2, gf2).wait_send()
    taken(1, 0, qk_in).wait_send()
    taken(1, 1, v_in).wait_send()
    taken(1, 2, m_in).wait_send()
    gather.close()


VM = pl.BlockSpec(memory_space=pltpu.VMEM)
SM = pl.BlockSpec(memory_space=pltpu.SMEM)
ANY = pl.BlockSpec(memory_space=pl.ANY)
DMA = pltpu.SemaphoreType.DMA


def per_device(
    context,
    latents,
    offsets,
    query_gain,
    key_gain,
    layer_gain,
    cross_query,
    cross_key,
    cross_value,
    cross_out,
    layer_qkv,
    layer_out,
):
    C, M = context.shape[1], latents.shape[1]
    R = M // N
    G = len(GROUPS)
    most = max(g[1] for g in GROUPS)
    return pl.pallas_call(
        kernel,
        out_shape=jax.ShapeDtypeStruct((1, R, D), BF),
        in_specs=[SM] + [ANY] * 11,
        out_specs=VM,
        scratch_shapes=[
            pltpu.VMEM((C, D), BF),
            pltpu.VMEM((M, D), BF),
            pltpu.VMEM((1, D), F32),
            pltpu.VMEM((1, D), F32),
            pltpu.VMEM((2, D), F32),
            pltpu.VMEM((24, K, K, K, 2, 8, HALF), BF),
            pltpu.VMEM(((K * K - 1) * most, 8, HALF), BF),
            pltpu.VMEM((C, D), BF),
            pltpu.VMEM((M, D), BF),
            pltpu.VMEM((H // 2, C, 128), BF),
            pltpu.VMEM((H // 2, C, 256), BF),
            pltpu.VMEM((H // 2, M, 128), BF),
            pltpu.VMEM((M, C), F32),
            pltpu.VMEM((H // 2, K, K, R, 128), BF),
            pltpu.VMEM((M, 128), F32),
            pltpu.VMEM((K, K, 8, 128), F32),
            pltpu.VMEM((2, K - 1, 4, K, R, 128), BF),
            pltpu.VMEM((2, K - 1, K, 8, 128), F32),
            pltpu.VMEM((2, 4, K, R, 128), BF),
            pltpu.VMEM((2, K, 8, 128), F32),
            pltpu.VMEM((2, K - 1, 4, R, 128), BF),
            pltpu.VMEM((2, K - 1, 8, 128), F32),
            pltpu.VMEM((R, D), BF),
            pltpu.VMEM((R, D), BF),
            pltpu.VMEM((R, D), BF),
            pltpu.VMEM((H, R, 128), BF),
            pltpu.VMEM((H, R // 2, 128), BF),
            pltpu.VMEM((2, N, R, 128), BF),
            pltpu.VMEM((2, N, R // 2, 128), BF),
            pltpu.VMEM((N, R // 2, 128), BF),
            pltpu.VMEM((2, H, R // 2, 128), BF),
            pltpu.VMEM((R, D), BF),
            DMA((5,)),
            DMA((24,)),
            DMA((G,)),
            DMA((G,)),
            DMA((G, 2)),
            DMA((G, 2)),
            DMA((G,)),
            DMA((G, 5)),
            DMA((4,)),
            DMA((4, 2, 3)),
            DMA((2, 3)),
            DMA((2, 3)),
        ],
        compiler_params=pltpu.CompilerParams(
            collective_id=0, has_side_effects=True, vmem_limit_bytes=60 << 20
        ),
        name="window",
    )(
        offsets, context, latents, query_gain[None], key_gain[None], layer_gain,
        cross_query, cross_key, cross_value, cross_out, layer_qkv, layer_out,
    )

def solution(mesh):
    return jax.shard_map(
        per_device,
        mesh=mesh,
        in_specs=(
            P("head", "seq", None),
            P("head", None, None),
            P("head"),
            P(),
            P(),
            P(),
            P(("seq", "head"), None),
            P(("seq", "head"), None),
            P(("seq", "head"), None),
            P(("seq", "head"), None),
            P(None, ("seq", "head"), None),
            P(None, ("seq", "head"), None),
        ),
        out_specs=P("head", "seq", None),
        check_vma=False,
    )
```
